1024 devices in a mesh: block: 64 (over z_lo, y, core), sub: 16 (over z_hi, x).
Axes of the slice: x: 4, y: 8, z: 16 (z_hi: 4, z_lo: 4; z = z_hi * 4 + z_lo), core: 2. Of those that a mesh axis runs over, the one named last changes fastest.
Arguments:
- source: float32 [64, 64, 128, 128], P('block', 'sub'), may hold values from -48 to 48
- trans_x: float32 [64, 64, 128, 128], P('block', 'sub'), may hold values from 0.1 to 10
- trans_y: float32 [64, 64, 128, 128], P('block', 'sub'), may hold values from 0.1 to 10
- trans_z: float32 [64, 64, 128, 128], P('block', 'sub'), may hold values from 0.1 to 10
- mortar_bot: float32 [64, 64, 128, 256], P('block', 'sub'), may hold values from -0.375 to 0.375
- mortar_top: float32 [64, 64, 128, 256], P('block', 'sub'), may hold values from -0.375 to 0.375
Outputs:
- pressure: float32 [64, 64, 128, 128], P('block', 'sub')
- mortar: float32 [64, 256], P('block', 'sub')
The draws below stay inside these ranges and needn't reach their ends.
All inputs are finite; a program needn't handle non-finite values.
Results may differ from the reference program's by a relative error of at most 0.0003.
Values sent between devices are 32-bit elements; how exact they have to be, the bound alone decides.
A program may use at most 32 MiB of HBM per device.

```python
import math
import jax
import jax.numpy as jnp
from jax import lax

NY = 128
CZ = 128
M = 256
PASSES = 3
OUTER = 2
NX = 64
N_BLOCK = 64


def block_levels(rng, extent, split, low, largest):
    def one(dim, blocks):
        steps = jax.random.uniform(jax.random.fold_in(jax.random.fold_in(rng, 6), dim), (blocks,), jnp.float32, low / len(split), largest / len(split))
        return jnp.repeat(jnp.exp(steps), extent[dim] // blocks).reshape((-1,) + (1,) * (len(extent) - dim - 1))

    level = one(*split[0])
    for cut in split[1:]:
        level = level * one(*cut)
    return level


def normal_values(key, extent, spread, limit, cuts=(), held_as=jnp.bfloat16):
    entries = spread * jax.random.normal(key, extent, jnp.float32)
    if cuts:
        entries = entries * block_levels(key, extent, cuts, -0.22, 0.18)
    return jnp.clip(entries, -limit, limit).astype(held_as)


def setup_inputs(seed: int = 0) -> dict:
    seeds = jax.random.split(jax.random.key(seed), 7)
    return {
        "source": normal_values(seeds[0], (N_BLOCK, NX, NY, CZ), 8.0, 48.0, ((0, 64), (1, 16)), jnp.float32),
        "trans_x": jnp.clip(jnp.exp(math.log(10.0) - 4.6051702 * jax.random.uniform(seeds[1], (N_BLOCK, NX, NY, CZ), jnp.float32) ** block_levels(seeds[1], (N_BLOCK, NX, NY, CZ), ((0, 64), (1, 16)), -0.2, 0.2)), 0.1, 10.0),
        "trans_y": jnp.clip(jnp.exp(math.log(10.0) - 4.6051702 * jax.random.uniform(seeds[2], (N_BLOCK, NX, NY, CZ), jnp.float32) ** block_levels(seeds[2], (N_BLOCK, NX, NY, CZ), ((0, 64), (1, 16)), -0.2, 0.2)), 0.1, 10.0),
        "trans_z": jnp.clip(jnp.exp(math.log(10.0) - 4.6051702 * jax.random.uniform(seeds[3], (N_BLOCK, NX, NY, CZ), jnp.float32) ** block_levels(seeds[3], (N_BLOCK, NX, NY, CZ), ((0, 64), (1, 16)), -0.2, 0.2)), 0.1, 10.0),
        "mortar_bot": normal_values(seeds[4], (N_BLOCK, NX, NY, M), M ** -0.5, 0.375, ((0, 64), (1, 16)), jnp.float32),
        "mortar_top": normal_values(seeds[5], (N_BLOCK, NX, NY, M), M ** -0.5, 0.375, ((0, 64), (1, 16)), jnp.float32),
    }


RELAX = 0.8
MORTAR_STEP = 0.05
HIGHEST = lax.Precision.HIGHEST


def below_of(values, axis):
    widths = [(0, 0)] * values.ndim
    widths[axis] = (1, 0)
    return lax.slice_in_dim(jnp.pad(values, widths), 0, values.shape[axis], axis=axis)


def above_of(values, axis):
    widths = [(0, 0)] * values.ndim
    widths[axis] = (0, 1)
    return lax.slice_in_dim(jnp.pad(values, widths), 1, values.shape[axis] + 1, axis=axis)


def reference(source, trans_x, trans_y, trans_z, mortar_bot, mortar_top):
    shape = source.shape
    blocks = shape[0]
    index_b = lax.broadcasted_iota(jnp.int32, shape, 0)
    index_x = lax.broadcasted_iota(jnp.int32, shape, 1)
    index_y = lax.broadcasted_iota(jnp.int32, shape, 2)
    index_z = lax.broadcasted_iota(jnp.int32, shape, 3)
    coupling_x = jnp.where(index_x > 0, trans_x, 0.0)
    coupling_y = jnp.where(index_y > 0, trans_y, 0.0)
    coupling_z = jnp.where(index_z > 0, trans_z, 0.0)
    dirichlet_bot = jnp.where((index_z == 0) & (index_b > 0), trans_z, 0.0)
    dirichlet_top = jnp.where((index_z == CZ - 1) & (index_b < blocks - 1), trans_z, 0.0)
    diagonal = (coupling_x + above_of(coupling_x, 1) + coupling_y + above_of(coupling_y, 2)
                + coupling_z + above_of(coupling_z, 3) + dirichlet_bot + dirichlet_top)
    face_bot = mortar_bot.reshape(blocks, NX * NY, M)
    face_top = mortar_top.reshape(blocks, NX * NY, M)
    pressure = jnp.zeros_like(source)
    mortar = jnp.zeros((blocks, M), source.dtype)
    for outer_round in range(OUTER):
        bottom_data = jnp.einsum("sfm,sm->sf", face_bot, below_of(mortar, 0), precision=HIGHEST).reshape(blocks, NX, NY)
        top_data = jnp.einsum("sfm,sm->sf", face_top, mortar, precision=HIGHEST).reshape(blocks, NX, NY)
        rhs = source + dirichlet_bot * bottom_data[..., None] + dirichlet_top * top_data[..., None]
        for pass_round in range(PASSES):
            applied = (diagonal * pressure
                       - coupling_x * below_of(pressure, 1) - above_of(coupling_x, 1) * above_of(pressure, 1)
                       - coupling_y * below_of(pressure, 2) - above_of(coupling_y, 2) * above_of(pressure, 2)
                       - coupling_z * below_of(pressure, 3) - above_of(coupling_z, 3) * above_of(pressure, 3))
            pressure = pressure + RELAX * (rhs - applied) / diagonal
        flux_bot = dirichlet_bot[..., 0] * (pressure[..., 0] - bottom_data)
        flux_top = dirichlet_top[..., CZ - 1] * (pressure[..., CZ - 1] - top_data)
        traces_bot = jnp.einsum("sfm,sf->sm", face_bot, flux_bot.reshape(blocks, NX * NY), precision=HIGHEST)
        traces_top = jnp.einsum("sfm,sf->sm", face_top, flux_top.reshape(blocks, NX * NY), precision=HIGHEST)
        mortar = mortar + MORTAR_STEP * (traces_top + above_of(traces_bot, 0))
    return pressure, mortar
```

```python
import functools
import jax
import jax.numpy as jnp
from jax import lax
from jax.experimental import pallas as pl
from jax.experimental.pallas import tpu as pltpu
from jax.sharding import PartitionSpec as P

RELAX = 0.8
MORTAR_STEP = 0.05
MESH = pl.DeviceIdType.MESH
GROUP = 4
CHUNKS = 4
F32 = jnp.float32


def roll(value, shift, axis):
    return pltpu.roll(value, shift % value.shape[axis], axis)


def kernel(
    sub_count, block_count,
    src_h, tx_h, ty_h, tz_h, mb_h, mt_h, p_out, m_out,
    src, tx, ty, tz, mb, mt,
    ayd, ayu, azd, azu, axd, axu, axh, face, wface, bias, press, pre, grid_g,
    d3, e1a, e1b, halo, cbuf, xr, zs, zr,
    load_sem, out_sem, e1_send, e1_recv, h_send, h_recv, x_send, x_recv, z_send, z_recv,
):
    layers, ny, nz = src.shape
    top = layers - 1
    mort = mb.shape[2]
    rows_m = mort // 128
    sub = lax.axis_index("sub")
    blk = lax.axis_index("block")
    xi = sub % GROUP
    zi = sub // GROUP
    zgroups = sub_count // GROUP
    has_low = sub > 0
    has_up = sub < sub_count - 1
    has_prev = blk > 0
    has_next = blk < block_count - 1
    rows_c = ny // CHUNKS

    loads = []
    for i, (h, v) in enumerate(((tx_h, tx), (ty_h, ty), (tz_h, tz), (src_h, src), (mb_h, mb), (mt_h, mt))):
        cp = pltpu.make_async_copy(h.at[0], v, load_sem.at[i])
        cp.start()
        loads.append(cp)

    barrier = pltpu.get_barrier_semaphore()

    def greet(b, s):
        pl.semaphore_signal(barrier, inc=1, device_id={"block": b, "sub": s}, device_id_type=MESH)

    def xpeer(j):
        return zi * GROUP + (xi + j) % GROUP

    slow_low = (xi == 0) & has_low
    slow_up = (xi == GROUP - 1) & has_up

    @pl.when(slow_low)
    def _():
        greet(blk, sub - 1)

    @pl.when(slow_up)
    def _():
        greet(blk, sub + 1)

    for j in range(1, GROUP):
        greet(blk, xpeer(j))
    for j in range(1, zgroups):
        greet(blk, (zi + j) % zgroups * GROUP + xi)

    @pl.when(has_prev)
    def _():
        for j in range(GROUP):
            greet(blk - 1, xpeer(j))

    @pl.when(has_next)
    def _():
        for j in range(GROUP):
            greet(blk + 1, xpeer(j))

    greeted = (
        GROUP - 1 + zgroups - 1
        + slow_low.astype(jnp.int32) + slow_up.astype(jnp.int32)
        + GROUP * has_prev.astype(jnp.int32) + GROUP * has_next.astype(jnp.int32)
    )

    zero_layer = jnp.zeros((ny, nz), F32)

    @pl.when(jnp.logical_not(has_low))
    def _():
        e1a[0] = zero_layer
        e1b[0] = zero_layer + 1.0
        for e in range(4):
            halo[e, 0] = zero_layer

    @pl.when(jnp.logical_not(has_up))
    def _():
        e1a[1] = zero_layer
        e1b[1] = zero_layer
        for e in range(4):
            halo[e, 1] = zero_layer

    zero_tile = jnp.zeros((8, 128), F32)
    for r in range(2):
        cbuf[r] = zero_tile
        zs[r] = zero_tile

    @pl.when(jnp.logical_not(has_next))
    def _():
        for r in range(2):
            for j in range(GROUP):
                xr[r, GROUP - 1 + j] = zero_tile

    @pl.when(jnp.logical_not(has_prev))
    def _():
        for r in range(2):
            for j in range(GROUP):
                xr[r, 2 * GROUP - 1 + j] = zero_tile

    iy = lax.broadcasted_iota(jnp.int32, (ny, nz), 0)
    iz = lax.broadcasted_iota(jnp.int32, (ny, nz), 1)
    bottom_cell = iz == 0
    top_cell = iz == nz - 1
    low_mask = has_low.astype(F32)
    prev_mask = has_prev.astype(F32)
    next_mask = has_next.astype(F32)

    loads[0].wait()
    loads[1].wait()
    loads[2].wait()
    loads[3].wait()

    def x_face(l):
        return tx[0] * low_mask if l == 0 else tx[l]

    def raw(l):
        cy = jnp.where(iy > 0, ty[l], 0.0)
        tzl = tz[l]
        cz = jnp.where(bottom_cell, 0.0, tzl)
        dirichlet = jnp.where(bottom_cell, tzl * prev_mask, 0.0) + jnp.where(top_cell, tzl * next_mask, 0.0)
        cyu = roll(cy, -1, 0)
        czu = roll(cz, -1, 1)
        return cy, cyu, cz, czu, dirichlet

    def keep(l, w, parts, low, up):
        cy, cyu, cz, czu, dirichlet = parts
        ayd[l] = w * cy
        ayu[l] = w * cyu
        azd[l] = w * cz
        azu[l] = w * czu
        wface[l] = w * dirichlet
        if l == 0:
            axh[0] = w * low
        else:
            axd[l] = w * low
        if l == top:
            axh[1] = w * up
        else:
            axu[l] = w * up
        b = w * src[l]
        bias[l] = b
        press[0, l] = b

    parts3 = raw(top)
    face[top] = parts3[4]
    d3[...] = x_face(top) + parts3[0] + parts3[1] + parts3[2] + parts3[3] + parts3[4]
    for l in range(top):
        parts = raw(l)
        face[l] = parts[4]
        low, up = x_face(l), tx[l + 1]
        diag = low + up + parts[0] + parts[1] + parts[2] + parts[3] + parts[4]
        keep(l, RELAX / diag, parts, low, up)

    pl.semaphore_wait(barrier, greeted)

    def e1_copy(i):
        source_ref, dest_ref, step = (
            (tx.at[0], e1a.at[1], -1),
            (press.at[0, 0], e1b.at[1], -1),
            (d3, e1b.at[0], 1),
            (src.at[top], e1a.at[0], 1),
        )[i]
        return pltpu.make_async_remote_copy(
            src_ref=source_ref, dst_ref=dest_ref, send_sem=e1_send.at[i], recv_sem=e1_recv.at[i],
            device_id={"block": blk, "sub": sub + step}, device_id_type=MESH,
        )

    @pl.when(has_low)
    def _():
        e1_copy(0).start()
        e1_copy(1).start()

    @pl.when(has_up)
    def _():
        e1_copy(2).start()
        e1_copy(3).start()

    def own_terms(k, l):
        p = press[k, l]
        return (
            (1.0 - RELAX) * p + bias[l]
            + ayd[l] * roll(p, 1, 0) + ayu[l] * roll(p, -1, 0)
            + azd[l] * roll(p, 1, 1) + azu[l] * roll(p, -1, 1)
        )

    def inner_layer(k, l):
        press[k + 1, l] = own_terms(k, l) + axd[l] * press[k, l - 1] + axu[l] * press[k, l + 1]

    def edge_terms(k, side):
        if side == 0:
            pre[0] = own_terms(k, 0) + axu[0] * press[k, 1]
        else:
            pre[1] = own_terms(k, top) + axd[top] * press[k, top - 1]

    def halo_copy(k, side, c):
        rows = pl.ds(c * rows_c, rows_c)
        return pltpu.make_async_remote_copy(
            src_ref=press.at[k, top * side, rows], dst_ref=halo.at[k - 1, 1 - side, rows],
            send_sem=h_send.at[k - 1, side, c], recv_sem=h_recv.at[k - 1, 1 - side, c],
            device_id={"block": blk, "sub": sub - 1 + 2 * side}, device_id_type=MESH,
        )

    def has(side):
        return jnp.where(side == 0, has_low.astype(jnp.int32), has_up.astype(jnp.int32)) > 0

    def send_side(k, side):
        @pl.when(has(side))
        def _():
            for c in range(CHUNKS):
                halo_copy(k, side, c).start()

    first_side = (xi != GROUP - 1).astype(jnp.int32)

    def edges(k, send):
        for t in range(2):
            side = first_side if t == 0 else 1 - first_side
            for c in range(CHUNKS):
                rows = pl.ds(c * rows_c, rows_c)

                @pl.when(has(side))
                def _():
                    halo_copy(k, 1 - side, c).wait_recv()

                press[k + 1, top * side, rows] = pre[side, rows] + axh[side, rows] * halo[k - 1, side, rows]
                if send:

                    @pl.when(has(side))
                    def _():
                        halo_copy(k + 1, side, c).start()

    inner_layer(0, 1)
    edge_terms(0, 0)

    @pl.when(has_up)
    def _():
        e1_copy(0).wait_recv()

    x_up = e1a[1]
    keep(top, RELAX / (d3[...] + x_up), raw(top), x_face(top), x_up)
    edge_terms(0, 1)

    @pl.when(has_up)
    def _():
        e1_copy(1).wait_recv()

    press[1, top] = pre[1] + axh[1] * e1b[1]
    send_side(1, 1)
    inner_layer(0, top - 1)

    @pl.when(has_low)
    def _():
        e1_copy(2).wait_recv()
        e1_copy(3).wait_recv()

    press[1, 0] = pre[0] + axh[0] * (RELAX * e1a[0] / (e1b[0] + x_face(0)))
    send_side(1, 0)

    def one_pass(k, send):
        for l in range(1, top):
            inner_layer(k, l)
        edge_terms(k, 0)
        edge_terms(k, 1)
        edges(k, send)

    one_pass(1, True)

    def project(k, with_g):
        acc_b = jnp.zeros((8, mort), F32)
        acc_t = jnp.zeros((8, mort), F32)
        for l in range(layers):
            p = press[k, l]
            f = face[l] * ((p - grid_g[l]) if with_g else p)
            fb = f[:, 0:1]
            ft = f[:, nz - 1 : nz]
            acc_b = acc_b + jnp.sum((fb * mb[l]).reshape(ny // 8, 8, mort), axis=0)
            acc_t = acc_t + jnp.sum((ft * mt[l]).reshape(ny // 8, 8, mort), axis=0)
        return jnp.sum(acc_t, axis=0, keepdims=True), jnp.sum(acc_b, axis=0, keepdims=True)

    def x_copy(r, i):
        if i < GROUP - 1:
            target = {"block": blk, "sub": xpeer(i + 1)}
        elif i < 2 * GROUP - 1:
            target = {"block": blk - 1, "sub": xpeer(i - GROUP + 1)}
        else:
            target = {"block": blk + 1, "sub": xpeer(i - 2 * GROUP + 1)}
        return pltpu.make_async_remote_copy(
            src_ref=cbuf.at[r], dst_ref=xr.at[r, i], send_sem=x_send.at[r, i], recv_sem=x_recv.at[r, i],
            device_id=target, device_id_type=MESH,
        )

    own = range(GROUP - 1)
    low_block = range(GROUP - 1, 2 * GROUP - 1)
    up_block = range(2 * GROUP - 1, 3 * GROUP - 1)

    def x_start(r, c_top, c_bot):
        for i in range(rows_m):
            cbuf[r, i : i + 1, :] = c_top[:, 128 * i : 128 * i + 128]
            cbuf[r, rows_m + i : rows_m + i + 1, :] = c_bot[:, 128 * i : 128 * i + 128]

        @pl.when(has_prev)
        def _():
            for i in low_block:
                x_copy(r, i).start()

        @pl.when(has_next)
        def _():
            for i in up_block:
                x_copy(r, i).start()

        for i in own:
            x_copy(r, i).start()

    def x_finish(r):
        for i in own:
            x_copy(r, i).wait_recv()

        @pl.when(has_next)
        def _():
            for i in low_block:
                x_copy(r, i).wait_recv()

        @pl.when(has_prev)
        def _():
            for i in up_block:
                x_copy(r, i).wait_recv()

        mine = cbuf[r]
        for i in own:
            mine = mine + xr[r, i]
        above = xr[r, low_block[0]]
        for i in low_block[1:]:
            above = above + xr[r, i]
        below = xr[r, up_block[0]]
        for i in up_block[1:]:
            below = below + xr[r, i]
        zs[r, 0:rows_m, :] = mine[0:rows_m] + above[rows_m : 2 * rows_m]
        zs[r, rows_m : 2 * rows_m, :] = below[0:rows_m] + mine[rows_m : 2 * rows_m]

    def z_copy(r, j):
        return pltpu.make_async_remote_copy(
            src_ref=zs.at[r], dst_ref=zr.at[r, j - 1], send_sem=z_send.at[r, j - 1], recv_sem=z_recv.at[r, j - 1],
            device_id={"block": blk, "sub": (zi + j) % zgroups * GROUP + xi}, device_id_type=MESH,
        )

    def z_start(r):
        for j in range(1, zgroups):
            z_copy(r, j).start()

    def z_finish(r):
        total = zs[r]
        for j in range(1, zgroups):
            z_copy(r, j).wait_recv()
            total = total + zr[r, j - 1]
        return MORTAR_STEP * total

    loads[4].wait()
    loads[5].wait()
    c_top, c_bot = project(2, False)
    x_start(0, c_top, c_bot)
    for l in range(1, top):
        inner_layer(2, l)
    edge_terms(2, 0)
    edge_terms(2, 1)
    x_finish(0)
    z_start(0)
    edges(2, False)
    mortar = z_finish(0)
    here = jnp.concatenate([mortar[i : i + 1, :] for i in range(rows_m)], axis=1)
    under = jnp.concatenate([mortar[rows_m + i : rows_m + i + 1, :] for i in range(rows_m)], axis=1)

    for l in (0, top) + tuple(range(1, top)):
        gb = jnp.sum(mb[l] * under, axis=1, keepdims=True)
        gt = jnp.sum(mt[l] * here, axis=1, keepdims=True)
        g = jnp.where(iz < nz // 2, gb, gt)
        grid_g[l] = g
        gain = wface[l] * g
        press[3, l] = press[3, l] + gain
        bias[l] = bias[l] + gain
        if l == 0:
            send_side(3, 0)
        if l == top:
            send_side(3, 1)

    one_pass(3, True)
    one_pass(4, False)

    out_copy = pltpu.make_async_copy(press.at[5], p_out.at[0], out_sem)
    out_copy.start()
    c_top, c_bot = project(5, True)
    x_start(1, c_top, c_bot)
    x_finish(1)
    z_start(1)
    final = mortar + z_finish(1)
    share = mort // sub_count
    offset = sub * share
    row = final[0:1, :]
    for i in range(1, rows_m):
        row = jnp.where(offset // 128 == i, final[i : i + 1, :], row)
    wide = jnp.broadcast_to(row, (8, 128))
    m_out[...] = pltpu.roll(wide, (128 - offset % 128) % 128, 1)[0:1, 0:share]

    out_copy.wait()

    @pl.when(has_low)
    def _():
        e1_copy(0).wait_send()
        e1_copy(1).wait_send()
        for k in range(1, 5):
            for c in range(CHUNKS):
                halo_copy(k, 0, c).wait_send()

    @pl.when(has_up)
    def _():
        e1_copy(2).wait_send()
        e1_copy(3).wait_send()
        for k in range(1, 5):
            for c in range(CHUNKS):
                halo_copy(k, 1, c).wait_send()

    for r in range(2):
        for i in own:
            x_copy(r, i).wait_send()
        for j in range(1, zgroups):
            z_copy(r, j).wait_send()

    @pl.when(has_prev)
    def _():
        for r in range(2):
            for i in low_block:
                x_copy(r, i).wait_send()

    @pl.when(has_next)
    def _():
        for r in range(2):
            for i in up_block:
                x_copy(r, i).wait_send()


def shards(source, trans_x, trans_y, trans_z, mortar_bot, mortar_top):
    _, layers, ny, nz = source.shape
    mort = mortar_bot.shape[3]
    sub_count = lax.axis_size("sub")
    block_count = lax.axis_size("block")
    zgroups = sub_count // GROUP
    field = pltpu.VMEM((layers, ny, nz), F32)
    basis = pltpu.VMEM((layers, ny, mort), F32)
    pair = pltpu.VMEM((2, ny, nz), F32)
    dma = pltpu.SemaphoreType.DMA
    xmsgs = 3 * GROUP - 1
    hbm = pl.BlockSpec(memory_space=pl.ANY)
    return pl.pallas_call(
        functools.partial(kernel, sub_count, block_count),
        out_shape=(
            jax.ShapeDtypeStruct(source.shape, F32),
            jax.ShapeDtypeStruct((1, mort // sub_count), F32),
        ),
        in_specs=[hbm] * 6,
        out_specs=(hbm, pl.BlockSpec(memory_space=pltpu.VMEM)),
        scratch_shapes=[
            field, field, field, field, basis, basis,
            field, field, field, field, field, field, pair, field, field, field,
            pltpu.VMEM((6, layers, ny, nz), F32), pair, field,
            pltpu.VMEM((ny, nz), F32), pair, pair, pltpu.VMEM((4, 2, ny, nz), F32),
            pltpu.VMEM((2, 8, 128), F32), pltpu.VMEM((2, xmsgs, 8, 128), F32),
            pltpu.VMEM((2, 8, 128), F32), pltpu.VMEM((2, zgroups - 1, 8, 128), F32),
            dma((6,)), dma, dma((4,)), dma((4,)),
            dma((4, 2, CHUNKS)), dma((4, 2, CHUNKS)),
            dma((2, xmsgs)), dma((2, xmsgs)), dma((2, zgroups - 1)), dma((2, zgroups - 1)),
        ],
        compiler_params=pltpu.CompilerParams(collective_id=0, has_side_effects=True),
        name="mortar_darcy",
    )(source, trans_x, trans_y, trans_z, mortar_bot, mortar_top)


def solution(mesh):
    spec = P("block", "sub", None, None)
    return jax.shard_map(
        shards,
        mesh=mesh,
        in_specs=(spec,) * 6,
        out_specs=(spec, P("block", "sub")),
        check_vma=False,
    )
```

```python
import functools
import jax
import jax.numpy as jnp
from jax import lax
from jax.experimental import pallas as pl
from jax.experimental.pallas import tpu as pltpu
from jax.sharding import PartitionSpec as P

RELAX = 0.8
MORTAR_STEP = 0.05
MESH = pl.DeviceIdType.MESH
GROUP = 4
CHUNKS = 4
RELAYED = {1: 3, 2: 0, 3: 3, 4: 0}
F32 = jnp.float32


def roll(value, shift, axis):
    return pltpu.roll(value, shift % value.shape[axis], axis)


def kernel(
    sub_count, block_count,
    src_h, tx_h, ty_h, tz_h, mb_h, mt_h, p_out, m_out,
    src, tx, ty, tz, mb, mt,
    ayd, ayu, azd, azu, axd, axu, axh, face, wface, bias, press, pre, grid_g, grid_d,
    d3, e1a, e1b, halo, cbuf, xr, zs, zr, part1, part, thin, thin_low, thin_up, g_own, g_halo,
    load_sem, e1_send, e1_recv, h_send, h_recv, x_send, x_recv, z_send, z_recv,
    p1_recv, f1_send, p_recv, f_send, t_send, t_recv, g_send, g_recv,
):
    layers, ny, nz = src.shape
    top = layers - 1
    mort = mb.shape[2]
    rows_m = mort // 128
    sub = lax.axis_index("sub")
    blk = lax.axis_index("block")
    xi = sub % GROUP
    zi = sub // GROUP
    zgroups = sub_count // GROUP
    has_low = sub > 0
    has_up = sub < sub_count - 1
    has_prev = blk > 0
    has_next = blk < block_count - 1
    rows_c = ny // CHUNKS
    rows_q = ny // GROUP
    first_x = xi == 0
    last_x = xi == GROUP - 1
    group_low = zi > 0
    group_up = zi < zgroups - 1
    inside_x = jnp.logical_not(first_x | last_x)

    loads = []
    for i, (h, v) in enumerate(((tx_h, tx), (ty_h, ty), (tz_h, tz), (src_h, src), (mb_h, mb), (mt_h, mt))):
        cp = pltpu.make_async_copy(h.at[0], v, load_sem.at[i])
        cp.start()
        loads.append(cp)

    barrier = pltpu.get_barrier_semaphore()

    def greet(b, s):
        pl.semaphore_signal(barrier, inc=1, device_id={"block": b, "sub": s}, device_id_type=MESH)

    def xpeer(j):
        return zi * GROUP + (xi + j) % GROUP

    slow_low = first_x & group_low
    slow_up = last_x & group_up
    pass_low = inside_x & group_low
    pass_up = inside_x & group_up

    @pl.when(slow_low)
    def _():
        for j in range(1, GROUP):
            greet(blk, sub - j)

    @pl.when(slow_up)
    def _():
        for j in range(1, GROUP):
            greet(blk, sub + j)

    @pl.when(pass_low)
    def _():
        greet(blk, (zi - 1) * GROUP + GROUP - 1)

    @pl.when(pass_up)
    def _():
        greet(blk, (zi + 1) * GROUP)

    for j in range(1, GROUP):
        greet(blk, xpeer(j))
    for j in range(1, zgroups):
        greet(blk, (zi + j) % zgroups * GROUP + xi)

    @pl.when(has_prev)
    def _():
        for j in range(GROUP):
            greet(blk - 1, xpeer(j))

    @pl.when(has_next)
    def _():
        for j in range(GROUP):
            greet(blk + 1, xpeer(j))

    greeted = (
        GROUP - 1 + zgroups - 1
        + (GROUP - 1) * (slow_low.astype(jnp.int32) + slow_up.astype(jnp.int32))
        + pass_low.astype(jnp.int32) + pass_up.astype(jnp.int32)
        + GROUP * has_prev.astype(jnp.int32) + GROUP * has_next.astype(jnp.int32)
    )

    zero_layer = jnp.zeros((ny, nz), F32)
    zero_thin = jnp.zeros((8, ny), F32)

    @pl.when(jnp.logical_not(has_low))
    def _():
        e1a[0] = zero_layer
        e1b[0] = zero_layer + 1.0
        for e in range(4):
            halo[e, 0] = zero_layer
        g_halo[0] = zero_thin
        for i in range(2):
            for f in range(3):
                thin_low[i, f] = zero_thin + 1.0

    @pl.when(jnp.logical_not(has_up))
    def _():
        e1a[1] = zero_layer
        e1b[1] = zero_layer
        for e in range(4):
            halo[e, 1] = zero_layer
        g_halo[1] = zero_thin
        for i in range(3):
            for f in range(3):
                thin_up[i, f] = zero_thin + (0.0 if i == 0 and f == 0 else 1.0)

    zero_tile = jnp.zeros((8, 128), F32)
    for r in range(2):
        cbuf[r] = zero_tile
        zs[r] = zero_tile

    @pl.when(jnp.logical_not(has_next))
    def _():
        for r in range(2):
            for j in range(GROUP):
                xr[r, GROUP - 1 + j] = zero_tile

    @pl.when(jnp.logical_not(has_prev))
    def _():
        for r in range(2):
            for j in range(GROUP):
                xr[r, 2 * GROUP - 1 + j] = zero_tile

    iy = lax.broadcasted_iota(jnp.int32, (ny, nz), 0)
    iz = lax.broadcasted_iota(jnp.int32, (ny, nz), 1)
    bottom_cell = iz == 0
    top_cell = iz == nz - 1
    low_mask = has_low.astype(F32)
    prev_mask = has_prev.astype(F32)
    next_mask = has_next.astype(F32)

    loads[0].wait()
    loads[1].wait()
    loads[2].wait()
    loads[3].wait()

    def x_face(l):
        return tx[0] * low_mask if l == 0 else tx[l]

    def raw(l):
        cy = jnp.where(iy > 0, ty[l], 0.0)
        tzl = tz[l]
        cz = jnp.where(bottom_cell, 0.0, tzl)
        dirichlet = jnp.where(bottom_cell, tzl * prev_mask, 0.0) + jnp.where(top_cell, tzl * next_mask, 0.0)
        cyu = roll(cy, -1, 0)
        czu = roll(cz, -1, 1)
        return cy, cyu, cz, czu, dirichlet

    def keep(l, w, parts, low, up):
        cy, cyu, cz, czu, dirichlet = parts
        ayd[l] = w * cy
        ayu[l] = w * cyu
        azd[l] = w * cz
        azu[l] = w * czu
        wface[l] = w * dirichlet
        if l == 0:
            axh[0] = w * low
        else:
            axd[l] = w * low
        if l == top:
            axh[1] = w * up
        else:
            axu[l] = w * up
        b = w * src[l]
        bias[l] = b
        press[0, l] = b

    parts3 = raw(top)
    face[top] = parts3[4]
    d3[...] = x_face(top) + parts3[0] + parts3[1] + parts3[2] + parts3[3] + parts3[4]
    for l in range(top):
        parts = raw(l)
        face[l] = parts[4]
        low, up = x_face(l), tx[l + 1]
        diag = low + up + parts[0] + parts[1] + parts[2] + parts[3] + parts[4]
        keep(l, RELAX / diag, parts, low, up)

    pl.semaphore_wait(barrier, greeted)

    def e1_copy(i, rows=None):
        source_ref, dest_ref, step = (
            (tx.at[0], e1a.at[1], -1),
            (press.at[0, 0], e1b.at[1], -1),
            (d3, e1b.at[0], 1),
            (src.at[top], e1a.at[0], 1),
        )[i]
        if rows is not None:
            source_ref, dest_ref = source_ref.at[rows], dest_ref.at[rows]
        return pltpu.make_async_remote_copy(
            src_ref=source_ref, dst_ref=dest_ref, send_sem=e1_send.at[i], recv_sem=e1_recv.at[i],
            device_id={"block": blk, "sub": sub + step}, device_id_type=MESH,
        )

    def e1_part(i, c):
        source_ref = (tx.at[0], press.at[0, 0], d3, src.at[top])[i]
        helper = (xi + c) % GROUP if i >= 2 else (xi + GROUP - c) % GROUP
        return pltpu.make_async_remote_copy(
            src_ref=source_ref.at[pl.ds(c * rows_q, rows_q)], dst_ref=part1.at[i],
            send_sem=e1_send.at[i], recv_sem=p1_recv.at[i],
            device_id={"block": blk, "sub": zi * GROUP + helper}, device_id_type=MESH,
        )

    def e1_forward(i):
        dest_ref = (e1a.at[1], e1b.at[1], e1b.at[0], e1a.at[0])[i]
        if i >= 2:
            c, target = (xi + 1) % GROUP, (zi + 1) * GROUP
        else:
            c, target = (GROUP - xi) % GROUP, (zi - 1) * GROUP + GROUP - 1
        return pltpu.make_async_remote_copy(
            src_ref=part1.at[i], dst_ref=dest_ref.at[pl.ds(c * rows_q, rows_q)],
            send_sem=f1_send.at[i], recv_sem=e1_recv.at[i],
            device_id={"block": blk, "sub": target}, device_id_type=MESH,
        )

    helps_low = jnp.logical_not(first_x) & group_low
    helps_up = jnp.logical_not(last_x) & group_up

    for across, pair in ((slow_low, (0, 1)), (slow_up, (2, 3))):

        @pl.when(across)
        def _():
            for c in (2, 1, 3):
                for i in pair:
                    e1_part(i, c).start()
            for i in pair:
                e1_copy(i, pl.ds(0, rows_q)).start()

    for beside, pair in ((jnp.logical_not(first_x), (0, 1)), (jnp.logical_not(last_x), (2, 3))):

        @pl.when(beside)
        def _():
            for i in pair:
                e1_copy(i).start()

    thin_row = lax.broadcasted_iota(jnp.int32, (8, ny), 0)
    thin_y = lax.broadcasted_iota(jnp.int32, (8, ny), 1)
    for l in range(layers):
        for f, ref in enumerate((tx, ty, tz)):
            turned = ref[l].T
            value = jnp.where(thin_row < 4, turned[0:8], turned[nz - 8 : nz])
            thin[l, f] = value * low_mask if l == 0 and f == 0 else value

    for helps, pair in ((helps_low, (0, 1)), (helps_up, (2, 3))):

        @pl.when(helps)
        def _():
            for i in pair:
                e1_part(i, 1).wait_recv()
                e1_forward(i).start()

    def own_terms(k, l):
        p = press[k, l]
        return (
            (1.0 - RELAX) * p + bias[l]
            + ayd[l] * roll(p, 1, 0) + ayu[l] * roll(p, -1, 0)
            + azd[l] * roll(p, 1, 1) + azu[l] * roll(p, -1, 1)
        )

    def inner_layer(k, l):
        press[k + 1, l] = own_terms(k, l) + axd[l] * press[k, l - 1] + axu[l] * press[k, l + 1]

    def edge_terms(k, side):
        if side == 0:
            pre[0] = own_terms(k, 0) + axu[0] * press[k, 1]
        else:
            pre[1] = own_terms(k, top) + axd[top] * press[k, top - 1]

    def halo_copy(k, side, c):
        rows = pl.ds(c * rows_c, rows_c)
        return pltpu.make_async_remote_copy(
            src_ref=press.at[k, top * side, rows], dst_ref=halo.at[k - 1, 1 - side, rows],
            send_sem=h_send.at[k - 1, side, c], recv_sem=h_recv.at[k - 1, 1 - side, c],
            device_id={"block": blk, "sub": sub - 1 + 2 * side}, device_id_type=MESH,
        )

    def part_copy(k, side):
        return pltpu.make_async_remote_copy(
            src_ref=press.at[k, top * side, pl.ds(RELAYED[k] * rows_c, rows_c)], dst_ref=part.at[k - 1],
            send_sem=h_send.at[k - 1, side, RELAYED[k]], recv_sem=p_recv.at[k - 1],
            device_id={"block": blk, "sub": sub + 1 - 2 * side}, device_id_type=MESH,
        )

    help_side = (xi == GROUP - 2).astype(jnp.int32)
    helps = ((xi == GROUP - 2) & group_up) | ((xi == 1) & group_low)

    def forward_copy(k):
        return pltpu.make_async_remote_copy(
            src_ref=part.at[k - 1],
            dst_ref=halo.at[k - 1, 1 - help_side, pl.ds(RELAYED[k] * rows_c, rows_c)],
            send_sem=f_send.at[k - 1], recv_sem=h_recv.at[k - 1, 1 - help_side, RELAYED[k]],
            device_id={"block": blk, "sub": (zi - 1 + 2 * help_side) * GROUP + (1 - help_side) * (GROUP - 1)},
            device_id_type=MESH,
        )

    def forward(k):
        if RELAYED[k] is None:
            return

        @pl.when(helps)
        def _():
            part_copy(k, help_side).wait_recv()
            forward_copy(k).start()

    def has(side):
        return jnp.where(side == 0, has_low.astype(jnp.int32), has_up.astype(jnp.int32)) > 0

    def slow(side):
        return jnp.where(side == 0, first_x.astype(jnp.int32), last_x.astype(jnp.int32)) > 0

    def send_chunk(k, side, c):
        if c != RELAYED[k]:

            @pl.when(has(side))
            def _():
                halo_copy(k, side, c).start()

        else:

            @pl.when(has(side) & jnp.logical_not(slow(side)))
            def _():
                halo_copy(k, side, c).start()

            @pl.when(has(side) & slow(side))
            def _():
                part_copy(k, side).start()

    def send_side(k, side):
        for c in sorted(range(CHUNKS), key=lambda c: c != RELAYED[k]):
            send_chunk(k, side, c)

    first_side = jnp.logical_not(last_x).astype(jnp.int32)

    def edges(k, send):
        for t in range(2):
            side = first_side if t == 0 else 1 - first_side
            for c in sorted(range(CHUNKS), key=lambda c: c == RELAYED[k]):
                rows = pl.ds(c * rows_c, rows_c)

                @pl.when(has(side))
                def _():
                    halo_copy(k, 1 - side, c).wait_recv()

                press[k + 1, top * side, rows] = pre[side, rows] + axh[side, rows] * halo[k - 1, side, rows]
                if send:
                    send_chunk(k + 1, side, c)

    inner_layer(0, 1)
    edge_terms(0, 0)

    def low_edge():
        @pl.when(has_low)
        def _():
            e1_copy(2).wait_recv()
            e1_copy(3).wait_recv()

        press[1, 0] = pre[0] + axh[0] * (RELAX * e1a[0] / (e1b[0] + x_face(0)))
        send_side(1, 0)

    @pl.when(last_x)
    def _():
        low_edge()

    @pl.when(has_up)
    def _():
        e1_copy(0).wait_recv()

    x_up = e1a[1]
    keep(top, RELAX / (d3[...] + x_up), raw(top), x_face(top), x_up)
    edge_terms(0, 1)

    @pl.when(has_up)
    def _():
        e1_copy(1).wait_recv()

    press[1, top] = pre[1] + axh[1] * e1b[1]
    send_side(1, 1)
    inner_layer(0, top - 1)

    @pl.when(jnp.logical_not(last_x))
    def _():
        low_edge()

    def one_pass(k, send):
        for l in range(1, top):
            inner_layer(k, l)
        edge_terms(k, 0)
        edge_terms(k, 1)
        edges(k, send)

    one_pass(1, True)
    forward(1)

    def thin_copy(side):
        low = side == 0
        return pltpu.make_async_remote_copy(
            src_ref=thin.at[0:3] if low else thin.at[layers - 2 : layers],
            dst_ref=thin_up if low else thin_low,
            send_sem=t_send.at[side], recv_sem=t_recv.at[1 - side],
            device_id={"block": blk, "sub": sub - 1 + 2 * side}, device_id_type=MESH,
        )

    def g_copy(side):
        return pltpu.make_async_remote_copy(
            src_ref=g_own, dst_ref=g_halo.at[1 - side], send_sem=g_send.at[side], recv_sem=g_recv.at[1 - side],
            device_id={"block": blk, "sub": sub - 1 + 2 * side}, device_id_type=MESH,
        )

    def on_sides(act):
        @pl.when(has_low)
        def _():
            act(0)

        @pl.when(has_up)
        def _():
            act(1)

    on_sides(lambda side: thin_copy(side).start())

    def project(acc, values, with_g):
        acc_t, acc_b = acc
        for l, p in values:
            f = face[l] * ((p - grid_g[l]) if with_g else p)
            fb = f[:, 0:1]
            ft = f[:, nz - 1 : nz]
            acc_b = acc_b + jnp.sum((fb * mb[l]).reshape(ny // 8, 8, mort), axis=0)
            acc_t = acc_t + jnp.sum((ft * mt[l]).reshape(ny // 8, 8, mort), axis=0)
        return acc_t, acc_b

    no_flux = (jnp.zeros((8, mort), F32), jnp.zeros((8, mort), F32))

    def x_copy(r, i):
        if i < GROUP - 1:
            target = {"block": blk, "sub": xpeer(i + 1)}
        elif i < 2 * GROUP - 1:
            target = {"block": blk - 1, "sub": xpeer(i - GROUP + 1)}
        else:
            target = {"block": blk + 1, "sub": xpeer(i - 2 * GROUP + 1)}
        return pltpu.make_async_remote_copy(
            src_ref=cbuf.at[r], dst_ref=xr.at[r, i], send_sem=x_send.at[r, i], recv_sem=x_recv.at[r, i],
            device_id=target, device_id_type=MESH,
        )

    own = range(GROUP - 1)
    low_block = range(GROUP - 1, 2 * GROUP - 1)
    up_block = range(2 * GROUP - 1, 3 * GROUP - 1)

    def x_start(r, acc):
        c_top, c_bot = (jnp.sum(v, axis=0, keepdims=True) for v in acc)
        for i in range(rows_m):
            cbuf[r, i : i + 1, :] = c_top[:, 128 * i : 128 * i + 128]
            cbuf[r, rows_m + i : rows_m + i + 1, :] = c_bot[:, 128 * i : 128 * i + 128]

        @pl.when(has_prev)
        def _():
            for i in low_block:
                x_copy(r, i).start()

        @pl.when(has_next)
        def _():
            for i in up_block:
                x_copy(r, i).start()

        for i in own:
            x_copy(r, i).start()

    def x_finish(r):
        for i in own:
            x_copy(r, i).wait_recv()

        @pl.when(has_next)
        def _():
            for i in low_block:
                x_copy(r, i).wait_recv()

        @pl.when(has_prev)
        def _():
            for i in up_block:
                x_copy(r, i).wait_recv()

        mine = cbuf[r]
        for i in own:
            mine = mine + xr[r, i]
        above = xr[r, low_block[0]]
        for i in low_block[1:]:
            above = above + xr[r, i]
        below = xr[r, up_block[0]]
        for i in up_block[1:]:
            below = below + xr[r, i]
        zs[r, 0:rows_m, :] = mine[0:rows_m] + above[rows_m : 2 * rows_m]
        zs[r, rows_m : 2 * rows_m, :] = below[0:rows_m] + mine[rows_m : 2 * rows_m]

    def z_copy(r, j):
        return pltpu.make_async_remote_copy(
            src_ref=zs.at[r], dst_ref=zr.at[r, j - 1], send_sem=z_send.at[r, j - 1], recv_sem=z_recv.at[r, j - 1],
            device_id={"block": blk, "sub": (zi + j) % zgroups * GROUP + xi}, device_id_type=MESH,
        )

    def z_start(r):
        for j in range(1, zgroups):
            z_copy(r, j).start()

    def z_finish(r):
        total = zs[r]
        for j in range(1, zgroups):
            z_copy(r, j).wait_recv()
            total = total + zr[r, j - 1]
        return MORTAR_STEP * total

    loads[4].wait()
    loads[5].wait()
    x_start(0, project(no_flux, [(l, press[2, l]) for l in range(layers)], False))
    for l in range(1, top):
        inner_layer(2, l)
    edge_terms(2, 0)
    edge_terms(2, 1)
    forward(2)
    x_finish(0)
    z_start(0)
    edges(2, True)
    forward(3)
    mortar = z_finish(0)
    here = jnp.concatenate([mortar[i : i + 1, :] for i in range(rows_m)], axis=1)
    under = jnp.concatenate([mortar[rows_m + i : rows_m + i + 1, :] for i in range(rows_m)], axis=1)

    columns = zero_layer
    for l in (0, top) + tuple(range(1, top)):
        gb = jnp.sum(mb[l] * under, axis=1, keepdims=True)
        gt = jnp.sum(mt[l] * here, axis=1, keepdims=True)
        columns = jnp.where(iz == l, gb, columns)
        columns = jnp.where(iz == layers + l, gt, columns)
        grid_g[l] = jnp.where(iz < nz // 2, gb, gt)
    g_own[...] = columns.T[0 : 2 * layers]
    on_sides(lambda side: g_copy(side).start())

    one_pass(3, True)
    forward(4)
    for l in range(1, top):
        inner_layer(4, l)
    edge_terms(4, 0)
    edge_terms(4, 1)

    on_sides(lambda side: thin_copy(1 - side).wait_recv())
    on_sides(lambda side: g_copy(1 - side).wait_recv())

    def thin_at(j, f):
        if j < 0:
            return thin_low[j + 2, f]
        return thin[j, f] if j < layers else thin_up[j - layers, f]

    def g_at(j):
        i = j % layers
        ref = g_halo.at[0] if j < 0 else g_own if j < layers else g_halo.at[1]
        return jnp.where(thin_row < 4, ref[i : i + 1, :], ref[layers + i : layers + i + 1, :])

    def thin_terms(j):
        low, up = thin_at(j, 0), thin_at(j + 1, 0)
        cy = jnp.where(thin_y > 0, thin_at(j, 1), 0.0)
        tzj = thin_at(j, 2)
        cz = jnp.where(thin_row > 0, tzj, 0.0)
        cyu = roll(cy, -1, 1)
        czu = roll(cz, -1, 0)
        dirichlet = jnp.where(thin_row == 0, tzj * prev_mask, 0.0) + jnp.where(thin_row == 7, tzj * next_mask, 0.0)
        w = RELAX / (low + up + cy + cyu + cz + czu + dirichlet)
        return w, low, up, cy, cyu, cz, czu, w * dirichlet * g_at(j)

    terms = {j: thin_terms(j) for j in range(-2, layers + 2)}

    def thin_pass(v, j):
        w, low, up, cy, cyu, cz, czu, b = terms[j]
        d = v[j]
        return (1.0 - RELAX) * d + b + w * (
            low * v[j - 1] + up * v[j + 1]
            + cy * roll(d, 1, 1) + cyu * roll(d, -1, 1) + cz * roll(d, 1, 0) + czu * roll(d, -1, 0)
        )

    first = {j: terms[j][7] for j in range(-2, layers + 2)}
    second = {j: thin_pass(first, j) for j in range(-1, layers + 1)}
    third = {j: thin_pass(second, j) for j in range(layers)}

    def added(l):
        d = third[l]
        tall = jnp.concatenate(
            [jnp.where(thin_row < 4, d, 0.0), jnp.zeros((nz - 16, ny), F32), jnp.where(thin_row < 4, 0.0, d)], axis=0
        )
        return tall.T

    def finish_layer(l):
        p = press[5, l] + grid_d[l]
        p_out[0, l] = p
        return l, p

    for l in range(layers):
        grid_d[l] = added(l)
    flux = project(no_flux, [finish_layer(l) for l in range(1, top)], True)
    edges(4, False)
    flux = project(flux, [finish_layer(l) for l in (0, top)], True)
    x_start(1, flux)
    x_finish(1)
    z_start(1)
    final = mortar + z_finish(1)
    share = mort // sub_count
    offset = sub * share
    row = final[0:1, :]
    for i in range(1, rows_m):
        row = jnp.where(offset // 128 == i, final[i : i + 1, :], row)
    wide = jnp.broadcast_to(row, (8, 128))
    m_out[...] = pltpu.roll(wide, (128 - offset % 128) % 128, 1)[0:1, 0:share]

    on_sides(lambda side: thin_copy(side).wait_send())
    on_sides(lambda side: g_copy(side).wait_send())

    @pl.when(has_low)
    def _():
        e1_copy(0).wait_send()
        e1_copy(1).wait_send()
        for k in range(1, 5):
            for c in range(CHUNKS):
                halo_copy(k, 0, c).wait_send()

    @pl.when(has_up)
    def _():
        e1_copy(2).wait_send()
        e1_copy(3).wait_send()
        for k in range(1, 5):
            for c in range(CHUNKS):
                halo_copy(k, 1, c).wait_send()

    @pl.when(helps_low)
    def _():
        e1_forward(0).wait_send()
        e1_forward(1).wait_send()

    @pl.when(helps_up)
    def _():
        e1_forward(2).wait_send()
        e1_forward(3).wait_send()

    @pl.when(helps)
    def _():
        for k in range(1, 5):
            if RELAYED[k] is not None:
                forward_copy(k).wait_send()

    for r in range(2):
        for i in own:
            x_copy(r, i).wait_send()
        for j in range(1, zgroups):
            z_copy(r, j).wait_send()

    @pl.when(has_prev)
    def _():
        for r in range(2):
            for i in low_block:
                x_copy(r, i).wait_send()

    @pl.when(has_next)
    def _():
        for r in range(2):
            for i in up_block:
                x_copy(r, i).wait_send()


def shards(source, trans_x, trans_y, trans_z, mortar_bot, mortar_top):
    _, layers, ny, nz = source.shape
    mort = mortar_bot.shape[3]
    sub_count = lax.axis_size("sub")
    block_count = lax.axis_size("block")
    zgroups = sub_count // GROUP
    field = pltpu.VMEM((layers, ny, nz), F32)
    basis = pltpu.VMEM((layers, ny, mort), F32)
    pair = pltpu.VMEM((2, ny, nz), F32)
    dma = pltpu.SemaphoreType.DMA
    xmsgs = 3 * GROUP - 1
    hbm = pl.BlockSpec(memory_space=pl.ANY)
    vmem = pl.BlockSpec(memory_space=pltpu.VMEM)
    return pl.pallas_call(
        functools.partial(kernel, sub_count, block_count),
        out_shape=(
            pltpu.VMEM(source.shape, F32),
            pltpu.VMEM((1, mort // sub_count), F32),
        ),
        in_specs=[hbm] * 6,
        out_specs=(vmem, vmem),
        scratch_shapes=[
            field, field, field, field, basis, basis,
            field, field, field, field, field, field, pair, field, field, field,
            pltpu.VMEM((6, layers, ny, nz), F32), pair, field, field,
            pltpu.VMEM((ny, nz), F32), pair, pair, pltpu.VMEM((4, 2, ny, nz), F32),
            pltpu.VMEM((2, 8, 128), F32), pltpu.VMEM((2, xmsgs, 8, 128), F32),
            pltpu.VMEM((2, 8, 128), F32), pltpu.VMEM((2, zgroups - 1, 8, 128), F32),
            pltpu.VMEM((4, ny // GROUP, nz), F32), pltpu.VMEM((4, ny // CHUNKS, nz), F32),
            pltpu.VMEM((layers, 3, 8, ny), F32), pltpu.VMEM((2, 3, 8, ny), F32), pltpu.VMEM((3, 3, 8, ny), F32),
            pltpu.VMEM((2 * layers, ny), F32), pltpu.VMEM((2, 2 * layers, ny), F32),
            dma((6,)), dma((4,)), dma((4,)),
            dma((4, 2, CHUNKS)), dma((4, 2, CHUNKS)),
            dma((2, xmsgs)), dma((2, xmsgs)), dma((2, zgroups - 1)), dma((2, zgroups - 1)),
            dma((4,)), dma((4,)), dma((4,)), dma((4,)),
            dma((2,)), dma((2,)), dma((2,)), dma((2,)),
        ],
        compiler_params=pltpu.CompilerParams(collective_id=0, has_side_effects=True),
        name="mortar_darcy",
    )(source, trans_x, trans_y, trans_z, mortar_bot, mortar_top)


def solution(mesh):
    spec = P("block", "sub", None, None)
    return jax.shard_map(
        shards,
        mesh=mesh,
        in_specs=(spec,) * 6,
        out_specs=(spec, P("block", "sub")),
        check_vma=False,
    )
```

```python
import functools
import jax
import jax.numpy as jnp
from jax import lax
from jax.experimental import pallas as pl
from jax.experimental.pallas import tpu as pltpu
from jax.sharding import PartitionSpec as P

RELAX = 0.8
MORTAR_STEP = 0.05
MESH = pl.DeviceIdType.MESH
GROUP = 4
CHUNKS = 4
RELAYED = {1: 3, 2: 0, 3: 3, 4: 0}
F32 = jnp.float32


def roll(value, shift, axis):
    return pltpu.roll(value, shift % value.shape[axis], axis)


def kernel(
    sub_count, block_count,
    src_h, tx_h, ty_h, tz_h, mb_h, mt_h, p_out, m_out,
    src, tx, ty, tz, mb, mt,
    ayd, ayu, azd, azu, axd, axu, axh, bias, press, pre, grid_d,
    d3, e1a, e1b, halo, cbuf, xr, zs, zr, part1, part, thin, thin_low, thin_up, near, near_low, near_up, g_own, g_halo,
    load_sem, e1_send, e1_recv, h_send, h_recv, x_send, x_recv, z_send, z_recv,
    p1_recv, f1_send, p_recv, f_send, t_send, t_recv, n_send, n_recv, g_send, g_recv,
):
    layers, ny, nz = src.shape
    top = layers - 1
    mort = mb.shape[2]
    rows_m = mort // 128
    sub = lax.axis_index("sub")
    blk = lax.axis_index("block")
    xi = sub % GROUP
    zi = sub // GROUP
    zgroups = sub_count // GROUP
    has_low = sub > 0
    has_up = sub < sub_count - 1
    has_prev = blk > 0
    has_next = blk < block_count - 1
    rows_c = ny // CHUNKS
    rows_q = ny // GROUP
    first_x = xi == 0
    last_x = xi == GROUP - 1
    group_low = zi > 0
    group_up = zi < zgroups - 1
    inside_x = jnp.logical_not(first_x | last_x)

    loads = []
    for i, (h, v) in enumerate(((tx_h, tx), (ty_h, ty), (tz_h, tz), (src_h, src), (mb_h, mb), (mt_h, mt))):
        cp = pltpu.make_async_copy(h.at[0], v, load_sem.at[i])
        cp.start()
        loads.append(cp)

    barrier = pltpu.get_barrier_semaphore()

    def greet(b, s):
        pl.semaphore_signal(barrier, inc=1, device_id={"block": b, "sub": s}, device_id_type=MESH)

    def xpeer(j):
        return zi * GROUP + (xi + j) % GROUP

    slow_low = first_x & group_low
    slow_up = last_x & group_up
    pass_low = inside_x & group_low
    pass_up = inside_x & group_up

    @pl.when(slow_low)
    def _():
        for j in range(1, GROUP):
            greet(blk, sub - j)

    @pl.when(slow_up)
    def _():
        for j in range(1, GROUP):
            greet(blk, sub + j)

    @pl.when(pass_low)
    def _():
        greet(blk, (zi - 1) * GROUP + GROUP - 1)

    @pl.when(pass_up)
    def _():
        greet(blk, (zi + 1) * GROUP)

    for j in range(1, GROUP):
        greet(blk, xpeer(j))
    for j in range(1, zgroups):
        greet(blk, (zi + j) % zgroups * GROUP + xi)

    @pl.when(has_prev)
    def _():
        for j in range(GROUP):
            greet(blk - 1, xpeer(j))

    @pl.when(has_next)
    def _():
        for j in range(GROUP):
            greet(blk + 1, xpeer(j))

    greeted = (
        GROUP - 1 + zgroups - 1
        + (GROUP - 1) * (slow_low.astype(jnp.int32) + slow_up.astype(jnp.int32))
        + pass_low.astype(jnp.int32) + pass_up.astype(jnp.int32)
        + GROUP * has_prev.astype(jnp.int32) + GROUP * has_next.astype(jnp.int32)
    )

    zero_layer = jnp.zeros((ny, nz), F32)
    zero_thin = jnp.zeros((8, ny), F32)

    @pl.when(jnp.logical_not(has_low))
    def _():
        e1a[0] = zero_layer
        e1b[0] = zero_layer + 1.0
        for e in range(4):
            halo[e, 0] = zero_layer
        g_halo[0] = zero_thin
        for i in range(2):
            for f in range(4):
                thin_low[i, f] = zero_thin + (0.0 if f == 3 else 1.0)
        for i in range(3):
            near_low[i] = zero_thin

    @pl.when(jnp.logical_not(has_up))
    def _():
        e1a[1] = zero_layer
        e1b[1] = zero_layer
        for e in range(4):
            halo[e, 1] = zero_layer
        g_halo[1] = zero_thin
        for i in range(3):
            for f in range(4):
                thin_up[i, f] = zero_thin + (0.0 if f == 3 or (i == 0 and f == 0) else 1.0)
        for i in range(3):
            near_up[i] = zero_thin

    zero_tile = jnp.zeros((8, 128), F32)
    for r in range(2):
        cbuf[r] = zero_tile
        zs[r] = zero_tile

    @pl.when(jnp.logical_not(has_next))
    def _():
        for r in range(2):
            for j in range(GROUP):
                xr[r, GROUP - 1 + j] = zero_tile

    @pl.when(jnp.logical_not(has_prev))
    def _():
        for r in range(2):
            for j in range(GROUP):
                xr[r, 2 * GROUP - 1 + j] = zero_tile

    iy = lax.broadcasted_iota(jnp.int32, (ny, nz), 0)
    iz = lax.broadcasted_iota(jnp.int32, (ny, nz), 1)
    bottom_cell = iz == 0
    top_cell = iz == nz - 1
    low_mask = has_low.astype(F32)
    prev_mask = has_prev.astype(F32)
    next_mask = has_next.astype(F32)

    loads[0].wait()
    loads[1].wait()
    loads[2].wait()
    loads[3].wait()

    def x_face(l):
        return tx[0] * low_mask if l == 0 else tx[l]

    def raw(l):
        cy = jnp.where(iy > 0, ty[l], 0.0)
        tzl = tz[l]
        cz = jnp.where(bottom_cell, 0.0, tzl)
        dirichlet = jnp.where(bottom_cell, tzl * prev_mask, 0.0) + jnp.where(top_cell, tzl * next_mask, 0.0)
        cyu = roll(cy, -1, 0)
        czu = roll(cz, -1, 1)
        return cy, cyu, cz, czu, dirichlet

    def keep(l, w, parts, low, up):
        cy, cyu, cz, czu, dirichlet = parts
        ayd[l] = w * cy
        ayu[l] = w * cyu
        azd[l] = w * cz
        azu[l] = w * czu
        if l == 0:
            axh[0] = w * low
        else:
            axd[l] = w * low
        if l == top:
            axh[1] = w * up
        else:
            axu[l] = w * up
        b = w * src[l]
        bias[l] = b
        press[0, l] = b

    parts3 = raw(top)
    d3[...] = x_face(top) + parts3[0] + parts3[1] + parts3[2] + parts3[3] + parts3[4]
    for l in range(top):
        parts = raw(l)
        low, up = x_face(l), tx[l + 1]
        diag = low + up + parts[0] + parts[1] + parts[2] + parts[3] + parts[4]
        keep(l, RELAX / diag, parts, low, up)

    thin_row = lax.broadcasted_iota(jnp.int32, (8, ny), 0)
    thin_y = lax.broadcasted_iota(jnp.int32, (8, ny), 1)

    def thinned(layer):
        turned = layer.T
        return jnp.where(thin_row < 4, turned[0:8], turned[nz - 8 : nz])

    for l in range(layers):
        for f, ref in enumerate((tx, ty, tz, src)):
            value = thinned(ref[l])
            thin[l, f] = value * low_mask if l == 0 and f == 0 else value

    pl.semaphore_wait(barrier, greeted)

    def on_sides(act):
        @pl.when(has_low)
        def _():
            act(0)

        @pl.when(has_up)
        def _():
            act(1)

    def side_copy(side, source_ref, dest_ref, send_sem, recv_sem):
        return pltpu.make_async_remote_copy(
            src_ref=source_ref, dst_ref=dest_ref, send_sem=send_sem, recv_sem=recv_sem,
            device_id={"block": blk, "sub": sub - 1 + 2 * side}, device_id_type=MESH,
        )

    def thin_copies(side):
        if side == 0:
            return (
                side_copy(0, thin.at[0:2], thin_up.at[0:2], t_send.at[0], t_recv.at[0]),
                side_copy(0, thin.at[2, 0], thin_up.at[2, 0], t_send.at[1], t_recv.at[1]),
            )
        return (side_copy(1, thin.at[layers - 2 : layers], thin_low, t_send.at[2], t_recv.at[2]),)

    def near_copy(side):
        if side == 0:
            return side_copy(0, near.at[0:3], near_up, n_send.at[0], n_recv.at[0])
        return side_copy(1, near.at[layers - 3 : layers], near_low, n_send.at[1], n_recv.at[1])

    def g_copy(side):
        return side_copy(side, g_own, g_halo.at[1 - side], g_send.at[side], g_recv.at[1 - side])

    def start_all(copies):
        for copy in copies:
            copy.start()

    on_sides(lambda side: start_all(thin_copies(side)))

    def e1_copy(i, rows=None):
        source_ref, dest_ref, step = (
            (tx.at[0], e1a.at[1], -1),
            (press.at[0, 0], e1b.at[1], -1),
            (d3, e1b.at[0], 1),
            (src.at[top], e1a.at[0], 1),
        )[i]
        if rows is not None:
            source_ref, dest_ref = source_ref.at[rows], dest_ref.at[rows]
        return pltpu.make_async_remote_copy(
            src_ref=source_ref, dst_ref=dest_ref, send_sem=e1_send.at[i], recv_sem=e1_recv.at[i],
            device_id={"block": blk, "sub": sub + step}, device_id_type=MESH,
        )

    def e1_part(i, c):
        source_ref = (tx.at[0], press.at[0, 0], d3, src.at[top])[i]
        helper = (xi + c) % GROUP if i >= 2 else (xi + GROUP - c) % GROUP
        return pltpu.make_async_remote_copy(
            src_ref=source_ref.at[pl.ds(c * rows_q, rows_q)], dst_ref=part1.at[i],
            send_sem=e1_send.at[i], recv_sem=p1_recv.at[i],
            device_id={"block": blk, "sub": zi * GROUP + helper}, device_id_type=MESH,
        )

    def e1_forward(i):
        dest_ref = (e1a.at[1], e1b.at[1], e1b.at[0], e1a.at[0])[i]
        if i >= 2:
            c, target = (xi + 1) % GROUP, (zi + 1) * GROUP
        else:
            c, target = (GROUP - xi) % GROUP, (zi - 1) * GROUP + GROUP - 1
        return pltpu.make_async_remote_copy(
            src_ref=part1.at[i], dst_ref=dest_ref.at[pl.ds(c * rows_q, rows_q)],
            send_sem=f1_send.at[i], recv_sem=e1_recv.at[i],
            device_id={"block": blk, "sub": target}, device_id_type=MESH,
        )

    helps_low = jnp.logical_not(first_x) & group_low
    helps_up = jnp.logical_not(last_x) & group_up

    for across, pair in ((slow_low, (0, 1)), (slow_up, (2, 3))):

        @pl.when(across)
        def _():
            for c in (2, 1, 3):
                for i in pair:
                    e1_part(i, c).start()
            for i in pair:
                e1_copy(i, pl.ds(0, rows_q)).start()

    for beside, pair in ((jnp.logical_not(first_x), (0, 1)), (jnp.logical_not(last_x), (2, 3))):

        @pl.when(beside)
        def _():
            for i in pair:
                e1_copy(i).start()

    for helps, pair in ((helps_low, (0, 1)), (helps_up, (2, 3))):

        @pl.when(helps)
        def _():
            for i in pair:
                e1_part(i, 1).wait_recv()
                e1_forward(i).start()

    def own_terms(k, l):
        p = press[k, l]
        return (
            (1.0 - RELAX) * p + bias[l]
            + ayd[l] * roll(p, 1, 0) + ayu[l] * roll(p, -1, 0)
            + azd[l] * roll(p, 1, 1) + azu[l] * roll(p, -1, 1)
        )

    def inner_layer(k, l):
        press[k + 1, l] = own_terms(k, l) + axd[l] * press[k, l - 1] + axu[l] * press[k, l + 1]

    def edge_terms(k, side):
        if side == 0:
            pre[0] = own_terms(k, 0) + axu[0] * press[k, 1]
        else:
            pre[1] = own_terms(k, top) + axd[top] * press[k, top - 1]

    def halo_copy(k, side, c):
        rows = pl.ds(c * rows_c, rows_c)
        return pltpu.make_async_remote_copy(
            src_ref=press.at[k, top * side, rows], dst_ref=halo.at[k - 1, 1 - side, rows],
            send_sem=h_send.at[k - 1, side, c], recv_sem=h_recv.at[k - 1, 1 - side, c],
            device_id={"block": blk, "sub": sub - 1 + 2 * side}, device_id_type=MESH,
        )

    def part_copy(k, side):
        return pltpu.make_async_remote_copy(
            src_ref=press.at[k, top * side, pl.ds(RELAYED[k] * rows_c, rows_c)], dst_ref=part.at[k - 1],
            send_sem=h_send.at[k - 1, side, RELAYED[k]], recv_sem=p_recv.at[k - 1],
            device_id={"block": blk, "sub": sub + 1 - 2 * side}, device_id_type=MESH,
        )

    help_side = (xi == GROUP - 2).astype(jnp.int32)
    helps = ((xi == GROUP - 2) & group_up) | ((xi == 1) & group_low)

    def forward_copy(k):
        return pltpu.make_async_remote_copy(
            src_ref=part.at[k - 1],
            dst_ref=halo.at[k - 1, 1 - help_side, pl.ds(RELAYED[k] * rows_c, rows_c)],
            send_sem=f_send.at[k - 1], recv_sem=h_recv.at[k - 1, 1 - help_side, RELAYED[k]],
            device_id={"block": blk, "sub": (zi - 1 + 2 * help_side) * GROUP + (1 - help_side) * (GROUP - 1)},
            device_id_type=MESH,
        )

    def forward(k):
        if RELAYED[k] is None:
            return

        @pl.when(helps)
        def _():
            part_copy(k, help_side).wait_recv()
            forward_copy(k).start()

    def has(side):
        return jnp.where(side == 0, has_low.astype(jnp.int32), has_up.astype(jnp.int32)) > 0

    def slow(side):
        return jnp.where(side == 0, first_x.astype(jnp.int32), last_x.astype(jnp.int32)) > 0

    def send_chunk(k, side, c):
        if c != RELAYED[k]:

            @pl.when(has(side))
            def _():
                halo_copy(k, side, c).start()

        else:

            @pl.when(has(side) & jnp.logical_not(slow(side)))
            def _():
                halo_copy(k, side, c).start()

            @pl.when(has(side) & slow(side))
            def _():
                part_copy(k, side).start()

    def send_side(k, side):
        for c in sorted(range(CHUNKS), key=lambda c: c != RELAYED[k]):
            send_chunk(k, side, c)

    first_side = jnp.logical_not(last_x).astype(jnp.int32)

    def edges(k, send):
        for t in range(2):
            side = first_side if t == 0 else 1 - first_side
            for c in sorted(range(CHUNKS), key=lambda c: c == RELAYED[k]):
                rows = pl.ds(c * rows_c, rows_c)

                @pl.when(has(side))
                def _():
                    halo_copy(k, 1 - side, c).wait_recv()

                press[k + 1, top * side, rows] = pre[side, rows] + axh[side, rows] * halo[k - 1, side, rows]
                if send:
                    send_chunk(k + 1, side, c)

    def x_copy(r, i):
        if i < GROUP - 1:
            target = {"block": blk, "sub": xpeer(i + 1)}
        elif i < 2 * GROUP - 1:
            target = {"block": blk - 1, "sub": xpeer(i - GROUP + 1)}
        else:
            target = {"block": blk + 1, "sub": xpeer(i - 2 * GROUP + 1)}
        return pltpu.make_async_remote_copy(
            src_ref=cbuf.at[r], dst_ref=xr.at[r, i], send_sem=x_send.at[r, i], recv_sem=x_recv.at[r, i],
            device_id=target, device_id_type=MESH,
        )

    own = range(GROUP - 1)
    low_block = range(GROUP - 1, 2 * GROUP - 1)
    up_block = range(2 * GROUP - 1, 3 * GROUP - 1)

    def x_start(r, acc):
        c_top, c_bot = (jnp.sum(v, axis=0, keepdims=True) for v in acc)
        for i in range(rows_m):
            cbuf[r, i : i + 1, :] = c_top[:, 128 * i : 128 * i + 128]
            cbuf[r, rows_m + i : rows_m + i + 1, :] = c_bot[:, 128 * i : 128 * i + 128]

        @pl.when(has_prev)
        def _():
            for i in low_block:
                x_copy(r, i).start()

        @pl.when(has_next)
        def _():
            for i in up_block:
                x_copy(r, i).start()

        for i in own:
            x_copy(r, i).start()

    def x_finish(r):
        for i in own:
            x_copy(r, i).wait_recv()

        @pl.when(has_next)
        def _():
            for i in low_block:
                x_copy(r, i).wait_recv()

        @pl.when(has_prev)
        def _():
            for i in up_block:
                x_copy(r, i).wait_recv()

        mine = cbuf[r]
        for i in own:
            mine = mine + xr[r, i]
        above = xr[r, low_block[0]]
        for i in low_block[1:]:
            above = above + xr[r, i]
        below = xr[r, up_block[0]]
        for i in up_block[1:]:
            below = below + xr[r, i]
        zs[r, 0:rows_m, :] = mine[0:rows_m] + above[rows_m : 2 * rows_m]
        zs[r, rows_m : 2 * rows_m, :] = below[0:rows_m] + mine[rows_m : 2 * rows_m]

    def z_copy(r, j):
        return pltpu.make_async_remote_copy(
            src_ref=zs.at[r], dst_ref=zr.at[r, j - 1], send_sem=z_send.at[r, j - 1], recv_sem=z_recv.at[r, j - 1],
            device_id={"block": blk, "sub": (zi + j) % zgroups * GROUP + xi}, device_id_type=MESH,
        )

    def z_start(r):
        for j in range(1, zgroups):
            z_copy(r, j).start()

    def z_finish(r):
        total = zs[r]
        for j in range(1, zgroups):
            z_copy(r, j).wait_recv()
            total = total + zr[r, j - 1]
        return MORTAR_STEP * total

    def project(fluxes):
        flat = jnp.concatenate([fluxes, jnp.zeros((128 - 2 * layers, ny), F32)], axis=0).T
        acc_t = jnp.zeros((8, mort), F32)
        acc_b = jnp.zeros((8, mort), F32)
        for l in range(layers):
            fb = flat[:, l : l + 1]
            ft = flat[:, layers + l : layers + l + 1]
            acc_b = acc_b + jnp.sum((fb * mb[l]).reshape(ny // 8, 8, mort), axis=0)
            acc_t = acc_t + jnp.sum((ft * mt[l]).reshape(ny // 8, 8, mort), axis=0)
        return acc_t, acc_b

    def face_rows(tiles):
        out = zero_thin
        for l in range(layers):
            out = jnp.where(thin_row == l, tiles[l][0:1, :], out)
            out = jnp.where(thin_row == layers + l, tiles[l][7:8, :], out)
        return out

    def thin_at(j, f):
        if j < 0:
            return thin_low[j + 2, f]
        return thin[j, f] if j < layers else thin_up[j - layers, f]

    def thin_terms(j):
        low, up = thin_at(j, 0), thin_at(j + 1, 0)
        cy = jnp.where(thin_y > 0, thin_at(j, 1), 0.0)
        tzj = thin_at(j, 2)
        cz = jnp.where(thin_row > 0, tzj, 0.0)
        cyu = roll(cy, -1, 1)
        czu = roll(cz, -1, 0)
        dirichlet = jnp.where(thin_row == 0, tzj * prev_mask, 0.0) + jnp.where(thin_row == 7, tzj * next_mask, 0.0)
        w = RELAX / (low + up + cy + cyu + cz + czu + dirichlet)
        return w, low, up, cy, cyu, cz, czu, dirichlet

    def thin_pass(terms, v, j, rhs):
        w, low, up, cy, cyu, cz, czu, _ = terms[j]
        d = v[j]
        return (1.0 - RELAX) * d + w * (
            rhs + low * v[j - 1] + up * v[j + 1]
            + cy * roll(d, 1, 1) + cyu * roll(d, -1, 1) + cz * roll(d, 1, 0) + czu * roll(d, -1, 0)
        )

    def low_edge():
        @pl.when(has_low)
        def _():
            e1_copy(2).wait_recv()
            e1_copy(3).wait_recv()

        press[1, 0] = pre[0] + axh[0] * (RELAX * e1a[0] / (e1b[0] + x_face(0)))
        send_side(1, 0)

    def up_edge():
        @pl.when(has_up)
        def _():
            e1_copy(0).wait_recv()

        x_up = e1a[1]
        keep(top, RELAX / (d3[...] + x_up), raw(top), x_face(top), x_up)
        edge_terms(0, 1)

        @pl.when(has_up)
        def _():
            e1_copy(1).wait_recv()

        press[1, top] = pre[1] + axh[1] * e1b[1]
        send_side(1, 1)

    inner_layer(0, 1)
    edge_terms(0, 0)

    @pl.when(last_x)
    def _():
        low_edge()

    @pl.when(jnp.logical_not(last_x))
    def _():
        up_edge()

    loads[4].wait()
    loads[5].wait()

    def wait_all(copies):
        for copy in copies:
            copy.wait_recv()

    on_sides(lambda side: wait_all(thin_copies(1 - side)))
    terms = {j: thin_terms(j) for j in range(-2, layers + 2)}
    level = {j: terms[j][0] * thin_at(j, 3) for j in terms}
    level = {j: thin_pass(terms, level, j, thin_at(j, 3)) for j in range(-1, layers + 1)}
    level = {j: thin_pass(terms, level, j, thin_at(j, 3)) for j in range(layers)}
    x_start(0, project(face_rows({l: terms[l][7] * level[l] for l in range(layers)})))

    @pl.when(last_x)
    def _():
        up_edge()

    @pl.when(jnp.logical_not(last_x))
    def _():
        low_edge()

    inner_layer(0, top - 1)
    forward(1)
    x_finish(0)
    z_start(0)

    def one_pass(k, send):
        for l in range(1, top):
            inner_layer(k, l)
        edge_terms(k, 0)
        edge_terms(k, 1)
        edges(k, send)

    one_pass(1, True)
    for l in range(layers):
        near[l] = thinned(press[2, l])
    on_sides(lambda side: near_copy(side).start())
    for l in range(1, top):
        inner_layer(2, l)
    edge_terms(2, 0)
    edge_terms(2, 1)
    forward(2)
    mortar = z_finish(0)
    here = jnp.concatenate([mortar[i : i + 1, :] for i in range(rows_m)], axis=1)
    under = jnp.concatenate([mortar[rows_m + i : rows_m + i + 1, :] for i in range(rows_m)], axis=1)

    columns = zero_layer
    for l in range(layers):
        gb = jnp.sum(mb[l] * under, axis=1, keepdims=True)
        gt = jnp.sum(mt[l] * here, axis=1, keepdims=True)
        columns = jnp.where(iz == l, gb, columns)
        columns = jnp.where(iz == layers + l, gt, columns)
    g_own[...] = columns.T[0 : 2 * layers]
    on_sides(lambda side: g_copy(side).start())

    edges(2, True)
    forward(3)
    for l in range(1, top):
        inner_layer(3, l)
    edge_terms(3, 0)
    edge_terms(3, 1)

    on_sides(lambda side: near_copy(1 - side).wait_recv())
    terms = {j: thin_terms(j) for j in range(-2, layers + 2)}
    level = {j: near_low[j + 3] if j < 0 else near[j] if j < layers else near_up[j - layers] for j in range(-3, layers + 3)}
    for width in (2, 1, 0):
        level = {j: thin_pass(terms, level, j, thin_at(j, 3)) for j in range(-width, layers + width)}

    on_sides(lambda side: g_copy(1 - side).wait_recv())

    def g_at(j):
        i = j % layers
        ref = g_halo.at[0] if j < 0 else g_own if j < layers else g_halo.at[1]
        return jnp.where(thin_row < 4, ref[i : i + 1, :], ref[layers + i : layers + i + 1, :])

    given = {j: terms[j][7] * g_at(j) for j in terms}
    extra = {j: terms[j][0] * given[j] for j in terms}
    for width in (1, 0):
        extra = {j: thin_pass(terms, extra, j, given[j]) for j in range(-width, layers + width)}
    x_start(1, project(face_rows({l: terms[l][7] * (level[l] + extra[l] - g_at(l)) for l in range(layers)})))

    def added(l):
        d = extra[l]
        tall = jnp.concatenate(
            [jnp.where(thin_row < 4, d, 0.0), jnp.zeros((nz - 16, ny), F32), jnp.where(thin_row < 4, 0.0, d)], axis=0
        )
        return tall.T

    for l in range(layers):
        grid_d[l] = added(l)

    edges(3, True)
    x_finish(1)
    z_start(1)
    forward(4)
    for l in range(1, top):
        inner_layer(4, l)
    edge_terms(4, 0)
    edge_terms(4, 1)
    for l in range(1, top):
        p_out[0, l] = press[5, l] + grid_d[l]
    edges(4, False)
    for l in (0, top):
        p_out[0, l] = press[5, l] + grid_d[l]
    final = mortar + z_finish(1)
    share = mort // sub_count
    offset = sub * share
    row = final[0:1, :]
    for i in range(1, rows_m):
        row = jnp.where(offset // 128 == i, final[i : i + 1, :], row)
    wide = jnp.broadcast_to(row, (8, 128))
    m_out[...] = pltpu.roll(wide, (128 - offset % 128) % 128, 1)[0:1, 0:share]

    def sent_all(copies):
        for copy in copies:
            copy.wait_send()

    on_sides(lambda side: sent_all(thin_copies(side)))
    on_sides(lambda side: near_copy(side).wait_send())
    on_sides(lambda side: g_copy(side).wait_send())

    @pl.when(has_low)
    def _():
        e1_copy(0).wait_send()
        e1_copy(1).wait_send()
        for k in range(1, 5):
            for c in range(CHUNKS):
                halo_copy(k, 0, c).wait_send()

    @pl.when(has_up)
    def _():
        e1_copy(2).wait_send()
        e1_copy(3).wait_send()
        for k in range(1, 5):
            for c in range(CHUNKS):
                halo_copy(k, 1, c).wait_send()

    @pl.when(helps_low)
    def _():
        e1_forward(0).wait_send()
        e1_forward(1).wait_send()

    @pl.when(helps_up)
    def _():
        e1_forward(2).wait_send()
        e1_forward(3).wait_send()

    @pl.when(helps)
    def _():
        for k in range(1, 5):
            if RELAYED[k] is not None:
                forward_copy(k).wait_send()

    for r in range(2):
        for i in own:
            x_copy(r, i).wait_send()
        for j in range(1, zgroups):
            z_copy(r, j).wait_send()

    @pl.when(has_prev)
    def _():
        for r in range(2):
            for i in low_block:
                x_copy(r, i).wait_send()

    @pl.when(has_next)
    def _():
        for r in range(2):
            for i in up_block:
                x_copy(r, i).wait_send()


def shards(source, trans_x, trans_y, trans_z, mortar_bot, mortar_top):
    _, layers, ny, nz = source.shape
    mort = mortar_bot.shape[3]
    sub_count = lax.axis_size("sub")
    block_count = lax.axis_size("block")
    zgroups = sub_count // GROUP
    field = pltpu.VMEM((layers, ny, nz), F32)
    basis = pltpu.VMEM((layers, ny, mort), F32)
    pair = pltpu.VMEM((2, ny, nz), F32)
    dma = pltpu.SemaphoreType.DMA
    xmsgs = 3 * GROUP - 1
    hbm = pl.BlockSpec(memory_space=pl.ANY)
    vmem = pl.BlockSpec(memory_space=pltpu.VMEM)
    return pl.pallas_call(
        functools.partial(kernel, sub_count, block_count),
        out_shape=(
            pltpu.VMEM(source.shape, F32),
            pltpu.VMEM((1, mort // sub_count), F32),
        ),
        in_specs=[hbm] * 6,
        out_specs=(vmem, vmem),
        scratch_shapes=[
            field, field, field, field, basis, basis,
            field, field, field, field, field, field, pair, field,
            pltpu.VMEM((6, layers, ny, nz), F32), pair, field,
            pltpu.VMEM((ny, nz), F32), pair, pair, pltpu.VMEM((4, 2, ny, nz), F32),
            pltpu.VMEM((2, 8, 128), F32), pltpu.VMEM((2, xmsgs, 8, 128), F32),
            pltpu.VMEM((2, 8, 128), F32), pltpu.VMEM((2, zgroups - 1, 8, 128), F32),
            pltpu.VMEM((4, ny // GROUP, nz), F32), pltpu.VMEM((4, ny // CHUNKS, nz), F32),
            pltpu.VMEM((layers, 4, 8, ny), F32), pltpu.VMEM((2, 4, 8, ny), F32), pltpu.VMEM((3, 4, 8, ny), F32),
            pltpu.VMEM((layers, 8, ny), F32), pltpu.VMEM((3, 8, ny), F32), pltpu.VMEM((3, 8, ny), F32),
            pltpu.VMEM((2 * layers, ny), F32), pltpu.VMEM((2, 2 * layers, ny), F32),
            dma((6,)), dma((4,)), dma((4,)),
            dma((4, 2, CHUNKS)), dma((4, 2, CHUNKS)),
            dma((2, xmsgs)), dma((2, xmsgs)), dma((2, zgroups - 1)), dma((2, zgroups - 1)),
            dma((4,)), dma((4,)), dma((4,)), dma((4,)),
            dma((3,)), dma((3,)), dma((2,)), dma((2,)), dma((2,)), dma((2,)),
        ],
        compiler_params=pltpu.CompilerParams(collective_id=0, has_side_effects=True),
        name="mortar_darcy",
    )(source, trans_x, trans_y, trans_z, mortar_bot, mortar_top)


def solution(mesh):
    spec = P("block", "sub", None, None)
    return jax.shard_map(
        shards,
        mesh=mesh,
        in_specs=(spec,) * 6,
        out_specs=(spec, P("block", "sub")),
        check_vma=False,
    )
```

```python
import functools
import jax
import jax.numpy as jnp
from jax import lax
from jax.experimental import pallas as pl
from jax.experimental.pallas import tpu as pltpu
from jax.sharding import PartitionSpec as P

RELAX = 0.8
MORTAR_STEP = 0.05
MESH = pl.DeviceIdType.MESH
GROUP = 4
CHUNKS = 4
RELAYED = {1: 3, 2: 0, 3: 3, 4: 0}
F32 = jnp.float32


def roll(value, shift, axis):
    return pltpu.roll(value, shift % value.shape[axis], axis)


def kernel(
    sub_count, block_count,
    src_h, tx_h, ty_h, tz_h, mb_h, mt_h, p_out, m_out,
    src, tx, ty, tz, mb, mt,
    ayd, ayu, azd, azu, axd, axu, axh, bias, press, pre, grid_d,
    d3, e1a, e1b, halo, cbuf, xr, zs, zr, part1, part, thin, thin_low, thin_up, near, near_low, near_up, g_own, g_halo,
    load_sem, e1_send, e1_recv, h_send, h_recv, x_send, x_recv, z_send, z_recv,
    p1_recv, f1_send, p_recv, f_send, t_send, t_recv, n_send, n_recv, g_send, g_recv, hello,
):
    layers, ny, nz = src.shape
    top = layers - 1
    mort = mb.shape[2]
    rows_m = mort // 128
    sub = lax.axis_index("sub")
    blk = lax.axis_index("block")
    xi = sub % GROUP
    zi = sub // GROUP
    zgroups = sub_count // GROUP
    has_low = sub > 0
    has_up = sub < sub_count - 1
    has_prev = blk > 0
    has_next = blk < block_count - 1
    rows_c = ny // CHUNKS
    rows_q = ny // GROUP
    first_x = xi == 0
    last_x = xi == GROUP - 1
    group_low = zi > 0
    group_up = zi < zgroups - 1
    inside_x = jnp.logical_not(first_x | last_x)

    loads = []
    for i, (h, v) in enumerate(((tx_h, tx), (ty_h, ty), (tz_h, tz), (src_h, src), (mb_h, mb), (mt_h, mt))):
        cp = pltpu.make_async_copy(h.at[0], v, load_sem.at[i])
        loads.append(cp)
        if i < 4:
            cp.start()

    barrier = pltpu.get_barrier_semaphore()

    def greet(b, s):
        pl.semaphore_signal(barrier, inc=1, device_id={"block": b, "sub": s}, device_id_type=MESH)

    def xpeer(j):
        return zi * GROUP + (xi + j) % GROUP

    slow_low = first_x & group_low
    slow_up = last_x & group_up
    pass_low = inside_x & group_low
    pass_up = inside_x & group_up

    @pl.when(slow_low)
    def _():
        for j in range(1, GROUP):
            greet(blk, sub - j)

    @pl.when(slow_up)
    def _():
        for j in range(1, GROUP):
            greet(blk, sub + j)

    @pl.when(pass_low)
    def _():
        greet(blk, (zi - 1) * GROUP + GROUP - 1)

    @pl.when(pass_up)
    def _():
        greet(blk, (zi + 1) * GROUP)

    for j in range(1, GROUP):
        greet(blk, xpeer(j))

    @pl.when(group_low)
    def _():
        greet(blk, sub - GROUP)

    @pl.when(group_up)
    def _():
        greet(blk, sub + GROUP)

    @pl.when(has_prev)
    def _():
        for j in range(GROUP):
            greet(blk - 1, xpeer(j))

    @pl.when(has_next)
    def _():
        for j in range(GROUP):
            greet(blk + 1, xpeer(j))

    greeted = (
        GROUP - 1 + group_low.astype(jnp.int32) + group_up.astype(jnp.int32)
        + (GROUP - 1) * (slow_low.astype(jnp.int32) + slow_up.astype(jnp.int32))
        + pass_low.astype(jnp.int32) + pass_up.astype(jnp.int32)
        + GROUP * has_prev.astype(jnp.int32) + GROUP * has_next.astype(jnp.int32)
    )

    zero_layer = jnp.zeros((ny, nz), F32)
    zero_thin = jnp.zeros((8, ny), F32)

    @pl.when(jnp.logical_not(has_low))
    def _():
        e1a[0] = zero_layer
        e1b[0] = zero_layer + 1.0
        for e in range(4):
            halo[e, 0] = zero_layer
        g_halo[0] = zero_thin
        for i in range(2):
            for f in range(4):
                thin_low[i, f] = zero_thin + (0.0 if f == 3 else 1.0)
        for i in range(3):
            near_low[i] = zero_thin

    @pl.when(jnp.logical_not(has_up))
    def _():
        e1a[1] = zero_layer
        e1b[1] = zero_layer
        for e in range(4):
            halo[e, 1] = zero_layer
        g_halo[1] = zero_thin
        for i in range(3):
            for f in range(4):
                thin_up[i, f] = zero_thin + (0.0 if f == 3 or (i == 0 and f == 0) else 1.0)
        for i in range(3):
            near_up[i] = zero_thin

    zero_tile = jnp.zeros((8, 128), F32)
    for r in range(2):
        cbuf[r] = zero_tile
        zs[r] = zero_tile

    @pl.when(jnp.logical_not(has_next))
    def _():
        for r in range(2):
            for j in range(GROUP):
                xr[r, GROUP - 1 + j] = zero_tile

    @pl.when(jnp.logical_not(has_prev))
    def _():
        for r in range(2):
            for j in range(GROUP):
                xr[r, 2 * GROUP - 1 + j] = zero_tile

    iy = lax.broadcasted_iota(jnp.int32, (ny, nz), 0)
    iz = lax.broadcasted_iota(jnp.int32, (ny, nz), 1)
    bottom_cell = iz == 0
    top_cell = iz == nz - 1
    low_mask = has_low.astype(F32)
    prev_mask = has_prev.astype(F32)
    next_mask = has_next.astype(F32)

    loads[0].wait()
    loads[1].wait()
    loads[2].wait()
    loads[3].wait()
    loads[4].start()
    loads[5].start()

    def x_face(l):
        return tx[0] * low_mask if l == 0 else tx[l]

    def raw(l):
        cy = jnp.where(iy > 0, ty[l], 0.0)
        tzl = tz[l]
        cz = jnp.where(bottom_cell, 0.0, tzl)
        dirichlet = jnp.where(bottom_cell, tzl * prev_mask, 0.0) + jnp.where(top_cell, tzl * next_mask, 0.0)
        cyu = roll(cy, -1, 0)
        czu = roll(cz, -1, 1)
        return cy, cyu, cz, czu, dirichlet

    def keep(l, w, parts, low, up):
        cy, cyu, cz, czu, dirichlet = parts
        ayd[l] = w * cy
        ayu[l] = w * cyu
        azd[l] = w * cz
        azu[l] = w * czu
        if l == 0:
            axh[0] = w * low
        else:
            axd[l] = w * low
        if l == top:
            axh[1] = w * up
        else:
            axu[l] = w * up
        b = w * src[l]
        bias[l] = b
        press[0, l] = b

    parts3 = raw(top)
    d3[...] = x_face(top) + parts3[0] + parts3[1] + parts3[2] + parts3[3] + parts3[4]

    def keep_low(l):
        parts = raw(l)
        low, up = x_face(l), tx[l + 1]
        diag = low + up + parts[0] + parts[1] + parts[2] + parts[3] + parts[4]
        keep(l, RELAX / diag, parts, low, up)

    keep_low(0)

    thin_row = lax.broadcasted_iota(jnp.int32, (8, ny), 0)
    thin_y = lax.broadcasted_iota(jnp.int32, (8, ny), 1)

    def thinned(layer):
        turned = layer.T
        return jnp.where(thin_row < 4, turned[0:8], turned[nz - 8 : nz])

    for l in range(layers):
        for f, ref in enumerate((tx, ty, tz, src)):
            value = thinned(ref[l])
            thin[l, f] = value * low_mask if l == 0 and f == 0 else value

    pl.semaphore_wait(barrier, greeted)

    def on_sides(act):
        @pl.when(has_low)
        def _():
            act(0)

        @pl.when(has_up)
        def _():
            act(1)

    def side_copy(side, source_ref, dest_ref, send_sem, recv_sem):
        return pltpu.make_async_remote_copy(
            src_ref=source_ref, dst_ref=dest_ref, send_sem=send_sem, recv_sem=recv_sem,
            device_id={"block": blk, "sub": sub - 1 + 2 * side}, device_id_type=MESH,
        )

    def thin_copies(side):
        if side == 0:
            return (
                side_copy(0, thin.at[0:2], thin_up.at[0:2], t_send.at[0], t_recv.at[0]),
                side_copy(0, thin.at[2, 0], thin_up.at[2, 0], t_send.at[1], t_recv.at[1]),
            )
        return (side_copy(1, thin.at[layers - 2 : layers], thin_low, t_send.at[2], t_recv.at[2]),)

    def near_copy(side):
        if side == 0:
            return side_copy(0, near.at[0:3], near_up, n_send.at[0], n_recv.at[0])
        return side_copy(1, near.at[layers - 3 : layers], near_low, n_send.at[1], n_recv.at[1])

    def g_copy(side):
        return side_copy(side, g_own, g_halo.at[1 - side], g_send.at[side], g_recv.at[1 - side])

    def start_all(copies):
        for copy in copies:
            copy.start()

    on_sides(lambda side: start_all(thin_copies(side)))

    def on_groups(act):
        @pl.when(group_low)
        def _():
            act(0)

        @pl.when(group_up)
        def _():
            act(1)

    def say_hello(r):
        def one(side):
            pl.semaphore_signal(
                hello.at[r, 1 - side], inc=1, device_id={"block": blk, "sub": sub - GROUP + 2 * GROUP * side},
                device_id_type=MESH,
            )

        if r < zgroups - 2:
            on_groups(one)

    def hear_hello(r):
        if r < zgroups - 2:
            on_groups(lambda side: pl.semaphore_wait(hello.at[r, side], 1))

    say_hello(0)

    def e1_copy(i, rows=None):
        source_ref, dest_ref, step = (
            (tx.at[0], e1a.at[1], -1),
            (press.at[0, 0], e1b.at[1], -1),
            (d3, e1b.at[0], 1),
            (src.at[top], e1a.at[0], 1),
        )[i]
        if rows is not None:
            source_ref, dest_ref = source_ref.at[rows], dest_ref.at[rows]
        return pltpu.make_async_remote_copy(
            src_ref=source_ref, dst_ref=dest_ref, send_sem=e1_send.at[i], recv_sem=e1_recv.at[i],
            device_id={"block": blk, "sub": sub + step}, device_id_type=MESH,
        )

    def e1_part(i, c):
        source_ref = (tx.at[0], press.at[0, 0], d3, src.at[top])[i]
        helper = (xi + c) % GROUP if i >= 2 else (xi + GROUP - c) % GROUP
        return pltpu.make_async_remote_copy(
            src_ref=source_ref.at[pl.ds(c * rows_q, rows_q)], dst_ref=part1.at[i],
            send_sem=e1_send.at[i], recv_sem=p1_recv.at[i],
            device_id={"block": blk, "sub": zi * GROUP + helper}, device_id_type=MESH,
        )

    def e1_forward(i):
        dest_ref = (e1a.at[1], e1b.at[1], e1b.at[0], e1a.at[0])[i]
        if i >= 2:
            c, target = (xi + 1) % GROUP, (zi + 1) * GROUP
        else:
            c, target = (GROUP - xi) % GROUP, (zi - 1) * GROUP + GROUP - 1
        return pltpu.make_async_remote_copy(
            src_ref=part1.at[i], dst_ref=dest_ref.at[pl.ds(c * rows_q, rows_q)],
            send_sem=f1_send.at[i], recv_sem=e1_recv.at[i],
            device_id={"block": blk, "sub": target}, device_id_type=MESH,
        )

    helps_low = jnp.logical_not(first_x) & group_low
    helps_up = jnp.logical_not(last_x) & group_up

    for across, pair in ((slow_low, (0, 1)), (slow_up, (2, 3))):

        @pl.when(across)
        def _():
            for c in (2, 1, 3):
                for i in pair:
                    e1_part(i, c).start()
            for i in pair:
                e1_copy(i, pl.ds(0, rows_q)).start()

    for beside, pair in ((jnp.logical_not(first_x), (0, 1)), (jnp.logical_not(last_x), (2, 3))):

        @pl.when(beside)
        def _():
            for i in pair:
                e1_copy(i).start()

    for l in range(1, top):
        keep_low(l)

    for helps, pair in ((helps_low, (0, 1)), (helps_up, (2, 3))):

        @pl.when(helps)
        def _():
            for i in pair:
                e1_part(i, 1).wait_recv()
                e1_forward(i).start()

    def own_terms(k, l):
        p = press[k, l]
        return (
            (1.0 - RELAX) * p + bias[l]
            + ayd[l] * roll(p, 1, 0) + ayu[l] * roll(p, -1, 0)
            + azd[l] * roll(p, 1, 1) + azu[l] * roll(p, -1, 1)
        )

    def inner_layer(k, l):
        press[k + 1, l] = own_terms(k, l) + axd[l] * press[k, l - 1] + axu[l] * press[k, l + 1]

    def edge_terms(k, side):
        if side == 0:
            pre[0] = own_terms(k, 0) + axu[0] * press[k, 1]
        else:
            pre[1] = own_terms(k, top) + axd[top] * press[k, top - 1]

    def halo_copy(k, side, c):
        rows = pl.ds(c * rows_c, rows_c)
        return pltpu.make_async_remote_copy(
            src_ref=press.at[k, top * side, rows], dst_ref=halo.at[k - 1, 1 - side, rows],
            send_sem=h_send.at[k - 1, side, c], recv_sem=h_recv.at[k - 1, 1 - side, c],
            device_id={"block": blk, "sub": sub - 1 + 2 * side}, device_id_type=MESH,
        )

    def part_copy(k, side):
        return pltpu.make_async_remote_copy(
            src_ref=press.at[k, top * side, pl.ds(RELAYED[k] * rows_c, rows_c)], dst_ref=part.at[k - 1],
            send_sem=h_send.at[k - 1, side, RELAYED[k]], recv_sem=p_recv.at[k - 1],
            device_id={"block": blk, "sub": sub + 1 - 2 * side}, device_id_type=MESH,
        )

    help_side = (xi == GROUP - 2).astype(jnp.int32)
    helps = ((xi == GROUP - 2) & group_up) | ((xi == 1) & group_low)

    def forward_copy(k):
        return pltpu.make_async_remote_copy(
            src_ref=part.at[k - 1],
            dst_ref=halo.at[k - 1, 1 - help_side, pl.ds(RELAYED[k] * rows_c, rows_c)],
            send_sem=f_send.at[k - 1], recv_sem=h_recv.at[k - 1, 1 - help_side, RELAYED[k]],
            device_id={"block": blk, "sub": (zi - 1 + 2 * help_side) * GROUP + (1 - help_side) * (GROUP - 1)},
            device_id_type=MESH,
        )

    def forward(k):
        if RELAYED[k] is None:
            return

        @pl.when(helps)
        def _():
            part_copy(k, help_side).wait_recv()
            forward_copy(k).start()

    def has(side):
        return jnp.where(side == 0, has_low.astype(jnp.int32), has_up.astype(jnp.int32)) > 0

    def slow(side):
        return jnp.where(side == 0, first_x.astype(jnp.int32), last_x.astype(jnp.int32)) > 0

    def send_chunk(k, side, c):
        if c != RELAYED[k]:

            @pl.when(has(side))
            def _():
                halo_copy(k, side, c).start()

        else:

            @pl.when(has(side) & jnp.logical_not(slow(side)))
            def _():
                halo_copy(k, side, c).start()

            @pl.when(has(side) & slow(side))
            def _():
                part_copy(k, side).start()

    def send_side(k, side):
        for c in sorted(range(CHUNKS), key=lambda c: c != RELAYED[k]):
            send_chunk(k, side, c)

    first_side = jnp.logical_not(last_x).astype(jnp.int32)

    def edges(k, send):
        for t in range(2):
            side = first_side if t == 0 else 1 - first_side
            for c in sorted(range(CHUNKS), key=lambda c: c == RELAYED[k]):
                rows = pl.ds(c * rows_c, rows_c)

                @pl.when(has(side))
                def _():
                    halo_copy(k, 1 - side, c).wait_recv()

                press[k + 1, top * side, rows] = pre[side, rows] + axh[side, rows] * halo[k - 1, side, rows]
                if send:
                    send_chunk(k + 1, side, c)

    def x_copy(r, i):
        if i < GROUP - 1:
            target = {"block": blk, "sub": xpeer(i + 1)}
        elif i < 2 * GROUP - 1:
            target = {"block": blk - 1, "sub": xpeer(i - GROUP + 1)}
        else:
            target = {"block": blk + 1, "sub": xpeer(i - 2 * GROUP + 1)}
        return pltpu.make_async_remote_copy(
            src_ref=cbuf.at[r], dst_ref=xr.at[r, i], send_sem=x_send.at[r, i], recv_sem=x_recv.at[r, i],
            device_id=target, device_id_type=MESH,
        )

    own = range(GROUP - 1)
    low_block = range(GROUP - 1, 2 * GROUP - 1)
    up_block = range(2 * GROUP - 1, 3 * GROUP - 1)

    def x_start(r, acc):
        c_top, c_bot = (jnp.sum(v, axis=0, keepdims=True) for v in acc)
        for i in range(rows_m):
            cbuf[r, i : i + 1, :] = c_top[:, 128 * i : 128 * i + 128]
            cbuf[r, rows_m + i : rows_m + i + 1, :] = c_bot[:, 128 * i : 128 * i + 128]

        @pl.when(has_prev)
        def _():
            for i in low_block:
                x_copy(r, i).start()

        @pl.when(has_next)
        def _():
            for i in up_block:
                x_copy(r, i).start()

        for i in own:
            x_copy(r, i).start()

    def x_finish(r):
        for i in own:
            x_copy(r, i).wait_recv()

        @pl.when(has_next)
        def _():
            for i in low_block:
                x_copy(r, i).wait_recv()

        @pl.when(has_prev)
        def _():
            for i in up_block:
                x_copy(r, i).wait_recv()

        mine = cbuf[r]
        for i in own:
            mine = mine + xr[r, i]
        above = xr[r, low_block[0]]
        for i in low_block[1:]:
            above = above + xr[r, i]
        below = xr[r, up_block[0]]
        for i in up_block[1:]:
            below = below + xr[r, i]
        zs[r, 0:rows_m, :] = mine[0:rows_m] + above[rows_m : 2 * rows_m]
        zs[r, rows_m : 2 * rows_m, :] = below[0:rows_m] + mine[rows_m : 2 * rows_m]

    def z_copy(r, j):
        return pltpu.make_async_remote_copy(
            src_ref=zs.at[r], dst_ref=zr.at[r, j - 1], send_sem=z_send.at[r, j - 1], recv_sem=z_recv.at[r, j - 1],
            device_id={"block": blk, "sub": (zi + j) % zgroups * GROUP + xi}, device_id_type=MESH,
        )

    def z_start(r):
        for j in range(1, zgroups):
            z_copy(r, j).start()

    def z_finish(r):
        total = zs[r]
        for j in range(1, zgroups):
            z_copy(r, j).wait_recv()
            total = total + zr[r, j - 1]
        return MORTAR_STEP * total

    def project(fluxes):
        flat = jnp.concatenate([fluxes, jnp.zeros((128 - 2 * layers, ny), F32)], axis=0).T
        acc_t = jnp.zeros((8, mort), F32)
        acc_b = jnp.zeros((8, mort), F32)
        for l in range(layers):
            fb = flat[:, l : l + 1]
            ft = flat[:, layers + l : layers + l + 1]
            acc_b = acc_b + jnp.sum((fb * mb[l]).reshape(ny // 8, 8, mort), axis=0)
            acc_t = acc_t + jnp.sum((ft * mt[l]).reshape(ny // 8, 8, mort), axis=0)
        return acc_t, acc_b

    def face_rows(tiles):
        out = zero_thin
        for l in range(layers):
            out = jnp.where(thin_row == l, tiles[l][0:1, :], out)
            out = jnp.where(thin_row == layers + l, tiles[l][7:8, :], out)
        return out

    def thin_at(j, f):
        if j < 0:
            return thin_low[j + 2, f]
        return thin[j, f] if j < layers else thin_up[j - layers, f]

    def thin_terms(j):
        low, up = thin_at(j, 0), thin_at(j + 1, 0)
        cy = jnp.where(thin_y > 0, thin_at(j, 1), 0.0)
        tzj = thin_at(j, 2)
        cz = jnp.where(thin_row > 0, tzj, 0.0)
        cyu = roll(cy, -1, 1)
        czu = roll(cz, -1, 0)
        dirichlet = jnp.where(thin_row == 0, tzj * prev_mask, 0.0) + jnp.where(thin_row == 7, tzj * next_mask, 0.0)
        w = RELAX / (low + up + cy + cyu + cz + czu + dirichlet)
        return w, low, up, cy, cyu, cz, czu, dirichlet

    def thin_pass(terms, v, j, rhs):
        w, low, up, cy, cyu, cz, czu, _ = terms[j]
        d = v[j]
        return (1.0 - RELAX) * d + w * (
            rhs + low * v[j - 1] + up * v[j + 1]
            + cy * roll(d, 1, 1) + cyu * roll(d, -1, 1) + cz * roll(d, 1, 0) + czu * roll(d, -1, 0)
        )

    def low_edge():
        @pl.when(has_low)
        def _():
            e1_copy(2).wait_recv()
            e1_copy(3).wait_recv()

        press[1, 0] = pre[0] + axh[0] * (RELAX * e1a[0] / (e1b[0] + x_face(0)))
        send_side(1, 0)

    def up_edge():
        @pl.when(has_up)
        def _():
            e1_copy(0).wait_recv()

        x_up = e1a[1]
        keep(top, RELAX / (d3[...] + x_up), raw(top), x_face(top), x_up)
        edge_terms(0, 1)

        @pl.when(has_up)
        def _():
            e1_copy(1).wait_recv()

        press[1, top] = pre[1] + axh[1] * e1b[1]
        send_side(1, 1)

    inner_layer(0, 1)
    edge_terms(0, 0)

    @pl.when(last_x)
    def _():
        low_edge()

    @pl.when(jnp.logical_not(last_x))
    def _():
        up_edge()

    loads[4].wait()
    loads[5].wait()

    def wait_all(copies):
        for copy in copies:
            copy.wait_recv()

    on_sides(lambda side: wait_all(thin_copies(1 - side)))
    terms = {j: thin_terms(j) for j in range(-2, layers + 2)}
    level = {j: terms[j][0] * thin_at(j, 3) for j in terms}
    level = {j: thin_pass(terms, level, j, thin_at(j, 3)) for j in range(-1, layers + 1)}
    level = {j: thin_pass(terms, level, j, thin_at(j, 3)) for j in range(layers)}
    x_start(0, project(face_rows({l: terms[l][7] * level[l] for l in range(layers)})))

    @pl.when(last_x)
    def _():
        up_edge()

    @pl.when(jnp.logical_not(last_x))
    def _():
        low_edge()

    inner_layer(0, top - 1)
    for r in range(zgroups - 2):
        hear_hello(r)
        say_hello(r + 1)
    forward(1)
    x_finish(0)
    z_start(0)

    def one_pass(k, send):
        for l in range(1, top):
            inner_layer(k, l)
        edge_terms(k, 0)
        edge_terms(k, 1)
        edges(k, send)

    one_pass(1, True)
    for l in range(layers):
        near[l] = thinned(press[2, l])
    on_sides(lambda side: near_copy(side).start())
    for l in range(1, top):
        inner_layer(2, l)
    edge_terms(2, 0)
    edge_terms(2, 1)
    forward(2)
    mortar = z_finish(0)
    here = jnp.concatenate([mortar[i : i + 1, :] for i in range(rows_m)], axis=1)
    under = jnp.concatenate([mortar[rows_m + i : rows_m + i + 1, :] for i in range(rows_m)], axis=1)

    columns = zero_layer
    for l in range(layers):
        gb = jnp.sum(mb[l] * under, axis=1, keepdims=True)
        gt = jnp.sum(mt[l] * here, axis=1, keepdims=True)
        columns = jnp.where(iz == l, gb, columns)
        columns = jnp.where(iz == layers + l, gt, columns)
    g_own[...] = columns.T[0 : 2 * layers]
    on_sides(lambda side: g_copy(side).start())

    edges(2, True)

    on_sides(lambda side: near_copy(1 - side).wait_recv())
    terms = {j: thin_terms(j) for j in range(-2, layers + 2)}
    level = {j: near_low[j + 3] if j < 0 else near[j] if j < layers else near_up[j - layers] for j in range(-3, layers + 3)}
    for width in (2, 1, 0):
        level = {j: thin_pass(terms, level, j, thin_at(j, 3)) for j in range(-width, layers + width)}

    on_sides(lambda side: g_copy(1 - side).wait_recv())

    def g_at(j):
        i = j % layers
        ref = g_halo.at[0] if j < 0 else g_own if j < layers else g_halo.at[1]
        return jnp.where(thin_row < 4, ref[i : i + 1, :], ref[layers + i : layers + i + 1, :])

    given = {j: terms[j][7] * g_at(j) for j in terms}
    extra = {j: terms[j][0] * given[j] for j in terms}
    for width in (1, 0):
        extra = {j: thin_pass(terms, extra, j, given[j]) for j in range(-width, layers + width)}
    x_start(1, project(face_rows({l: terms[l][7] * (level[l] + extra[l] - g_at(l)) for l in range(layers)})))

    def added(l):
        d = extra[l]
        tall = jnp.concatenate(
            [jnp.where(thin_row < 4, d, 0.0), jnp.zeros((nz - 16, ny), F32), jnp.where(thin_row < 4, 0.0, d)], axis=0
        )
        return tall.T

    for l in range(layers):
        grid_d[l] = added(l)

    for l in range(1, top):
        inner_layer(3, l)
    edge_terms(3, 0)
    edge_terms(3, 1)
    forward(3)
    x_finish(1)
    z_start(1)
    edges(3, True)
    forward(4)
    for l in range(1, top):
        inner_layer(4, l)
    edge_terms(4, 0)
    edge_terms(4, 1)
    for l in range(1, top):
        p_out[0, l] = press[5, l] + grid_d[l]
    edges(4, False)
    for l in (0, top):
        p_out[0, l] = press[5, l] + grid_d[l]
    final = mortar + z_finish(1)
    share = mort // sub_count
    offset = sub * share
    row = final[0:1, :]
    for i in range(1, rows_m):
        row = jnp.where(offset // 128 == i, final[i : i + 1, :], row)
    wide = jnp.broadcast_to(row, (8, 128))
    m_out[...] = pltpu.roll(wide, (128 - offset % 128) % 128, 1)[0:1, 0:share]

    def sent_all(copies):
        for copy in copies:
            copy.wait_send()

    on_sides(lambda side: sent_all(thin_copies(side)))
    on_sides(lambda side: near_copy(side).wait_send())
    on_sides(lambda side: g_copy(side).wait_send())

    @pl.when(has_low)
    def _():
        e1_copy(0).wait_send()
        e1_copy(1).wait_send()
        for k in range(1, 5):
            for c in range(CHUNKS):
                halo_copy(k, 0, c).wait_send()

    @pl.when(has_up)
    def _():
        e1_copy(2).wait_send()
        e1_copy(3).wait_send()
        for k in range(1, 5):
            for c in range(CHUNKS):
                halo_copy(k, 1, c).wait_send()

    @pl.when(helps_low)
    def _():
        e1_forward(0).wait_send()
        e1_forward(1).wait_send()

    @pl.when(helps_up)
    def _():
        e1_forward(2).wait_send()
        e1_forward(3).wait_send()

    @pl.when(helps)
    def _():
        for k in range(1, 5):
            if RELAYED[k] is not None:
                forward_copy(k).wait_send()

    for r in range(2):
        for i in own:
            x_copy(r, i).wait_send()
        for j in range(1, zgroups):
            z_copy(r, j).wait_send()

    @pl.when(has_prev)
    def _():
        for r in range(2):
            for i in low_block:
                x_copy(r, i).wait_send()

    @pl.when(has_next)
    def _():
        for r in range(2):
            for i in up_block:
                x_copy(r, i).wait_send()


def shards(source, trans_x, trans_y, trans_z, mortar_bot, mortar_top):
    _, layers, ny, nz = source.shape
    mort = mortar_bot.shape[3]
    sub_count = lax.axis_size("sub")
    block_count = lax.axis_size("block")
    zgroups = sub_count // GROUP
    field = pltpu.VMEM((layers, ny, nz), F32)
    basis = pltpu.VMEM((layers, ny, mort), F32)
    pair = pltpu.VMEM((2, ny, nz), F32)
    dma = pltpu.SemaphoreType.DMA
    xmsgs = 3 * GROUP - 1
    hbm = pl.BlockSpec(memory_space=pl.ANY)
    vmem = pl.BlockSpec(memory_space=pltpu.VMEM)
    return pl.pallas_call(
        functools.partial(kernel, sub_count, block_count),
        out_shape=(
            pltpu.VMEM(source.shape, F32),
            pltpu.VMEM((1, mort // sub_count), F32),
        ),
        in_specs=[hbm] * 6,
        out_specs=(vmem, vmem),
        scratch_shapes=[
            field, field, field, field, basis, basis,
            field, field, field, field, field, field, pair, field,
            pltpu.VMEM((6, layers, ny, nz), F32), pair, field,
            pltpu.VMEM((ny, nz), F32), pair, pair, pltpu.VMEM((4, 2, ny, nz), F32),
            pltpu.VMEM((2, 8, 128), F32), pltpu.VMEM((2, xmsgs, 8, 128), F32),
            pltpu.VMEM((2, 8, 128), F32), pltpu.VMEM((2, zgroups - 1, 8, 128), F32),
            pltpu.VMEM((4, ny // GROUP, nz), F32), pltpu.VMEM((4, ny // CHUNKS, nz), F32),
            pltpu.VMEM((layers, 4, 8, ny), F32), pltpu.VMEM((2, 4, 8, ny), F32), pltpu.VMEM((3, 4, 8, ny), F32),
            pltpu.VMEM((layers, 8, ny), F32), pltpu.VMEM((3, 8, ny), F32), pltpu.VMEM((3, 8, ny), F32),
            pltpu.VMEM((2 * layers, ny), F32), pltpu.VMEM((2, 2 * layers, ny), F32),
            dma((6,)), dma((4,)), dma((4,)),
            dma((4, 2, CHUNKS)), dma((4, 2, CHUNKS)),
            dma((2, xmsgs)), dma((2, xmsgs)), dma((2, zgroups - 1)), dma((2, zgroups - 1)),
            dma((4,)), dma((4,)), dma((4,)), dma((4,)),
            dma((3,)), dma((3,)), dma((2,)), dma((2,)), dma((2,)), dma((2,)),
            pltpu.SemaphoreType.REGULAR((max(zgroups - 2, 1), 2)),
        ],
        compiler_params=pltpu.CompilerParams(collective_id=0, has_side_effects=True),
        name="mortar_darcy",
    )(source, trans_x, trans_y, trans_z, mortar_bot, mortar_top)


def solution(mesh):
    spec = P("block", "sub", None, None)
    return jax.shard_map(
        shards,
        mesh=mesh,
        in_specs=(spec,) * 6,
        out_specs=(spec, P("block", "sub")),
        check_vma=False,
    )
```

```python
import functools
import jax
import jax.numpy as jnp
from jax import lax
from jax.experimental import pallas as pl
from jax.experimental.pallas import tpu as pltpu
from jax.sharding import PartitionSpec as P

RELAX = 0.8
MORTAR_STEP = 0.05
MESH = pl.DeviceIdType.MESH
GROUP = 4
CHUNKS = 4
RELAYED = {1: 3, 2: 0, 3: 3, 4: 0}
F32 = jnp.float32


def roll(value, shift, axis):
    return pltpu.roll(value, shift % value.shape[axis], axis)


def kernel(
    sub_count, block_count,
    src_h, tx_h, ty_h, tz_h, mb_h, mt_h, p_out, m_out,
    src, tx, ty, tz, mb, mt,
    ayd, ayu, azd, azu, axd, axu, axh, bias, press, pre, grid_d,
    d3, e1a, e1b, halo, cbuf, xr, zs, zr, part1, part, thin, thin_low, thin_up, near, near_low, near_up, g_own, g_halo,
    load_sem, e1_send, e1_recv, h_send, h_recv, x_send, x_recv, z_send, z_recv,
    p1_recv, f1_send, p_recv, f_send, t_send, t_recv, n_send, n_recv, g_send, g_recv, hello,
):
    layers, ny, nz = src.shape
    top = layers - 1
    mort = mb.shape[2]
    rows_m = mort // 128
    sub = lax.axis_index("sub")
    blk = lax.axis_index("block")
    xi = sub % GROUP
    zi = sub // GROUP
    zgroups = sub_count // GROUP
    has_low = sub > 0
    has_up = sub < sub_count - 1
    has_prev = blk > 0
    has_next = blk < block_count - 1
    rows_c = ny // CHUNKS
    rows_q = (ny - 8) // (GROUP - 1)

    def quarter(c):
        return pl.ds(8 + (c - 1) * rows_q, rows_q)

    first_x = xi == 0
    last_x = xi == GROUP - 1
    group_low = zi > 0
    group_up = zi < zgroups - 1
    inside_x = jnp.logical_not(first_x | last_x)

    loads = []
    for i, (h, v) in enumerate(((tx_h, tx), (ty_h, ty), (tz_h, tz), (src_h, src), (mb_h, mb), (mt_h, mt))):
        cp = pltpu.make_async_copy(h.at[0], v, load_sem.at[i])
        loads.append(cp)
        if i < 4:
            cp.start()

    barrier = pltpu.get_barrier_semaphore()

    def greet(b, s):
        pl.semaphore_signal(barrier, inc=1, device_id={"block": b, "sub": s}, device_id_type=MESH)

    def xpeer(j):
        return zi * GROUP + (xi + j) % GROUP

    slow_low = first_x & group_low
    slow_up = last_x & group_up
    pass_low = inside_x & group_low
    pass_up = inside_x & group_up

    @pl.when(slow_low)
    def _():
        for j in range(1, GROUP):
            greet(blk, sub - j)

    @pl.when(slow_up)
    def _():
        for j in range(1, GROUP):
            greet(blk, sub + j)

    @pl.when(pass_low)
    def _():
        greet(blk, (zi - 1) * GROUP + GROUP - 1)

    @pl.when(pass_up)
    def _():
        greet(blk, (zi + 1) * GROUP)

    for j in range(1, GROUP):
        greet(blk, xpeer(j))

    @pl.when(group_low & jnp.logical_not(first_x))
    def _():
        greet(blk, sub - GROUP)

    @pl.when(group_up)
    def _():
        greet(blk, sub + GROUP)

    @pl.when(has_prev)
    def _():
        for j in range(GROUP):
            greet(blk - 1, xpeer(j))

    @pl.when(has_next)
    def _():
        for j in range(GROUP):
            greet(blk + 1, xpeer(j))

    greeted = (
        GROUP - 1 + group_low.astype(jnp.int32) + (group_up & jnp.logical_not(first_x)).astype(jnp.int32)
        + (GROUP - 1) * (slow_low.astype(jnp.int32) + slow_up.astype(jnp.int32))
        + pass_low.astype(jnp.int32) + pass_up.astype(jnp.int32)
        + GROUP * has_prev.astype(jnp.int32) + GROUP * has_next.astype(jnp.int32)
    )

    zero_layer = jnp.zeros((ny, nz), F32)
    zero_thin = jnp.zeros((8, ny), F32)

    @pl.when(jnp.logical_not(has_low))
    def _():
        e1a[0] = zero_layer
        e1b[0] = zero_layer + 1.0
        for e in range(4):
            halo[e, 0] = zero_layer
        g_halo[0] = zero_thin
        for i in range(2):
            for f in range(4):
                thin_low[i, f] = zero_thin + (0.0 if f == 3 else 1.0)
        for i in range(3):
            near_low[i] = zero_thin

    @pl.when(jnp.logical_not(has_up))
    def _():
        e1a[1] = zero_layer
        e1b[1] = zero_layer
        for e in range(4):
            halo[e, 1] = zero_layer
        g_halo[1] = zero_thin
        for i in range(3):
            for f in range(4):
                thin_up[i, f] = zero_thin + (0.0 if f == 3 or (i == 0 and f == 0) else 1.0)
        for i in range(3):
            near_up[i] = zero_thin

    zero_tile = jnp.zeros((8, 128), F32)
    for r in range(2):
        cbuf[r] = zero_tile
        zs[r] = zero_tile

    @pl.when(jnp.logical_not(has_next))
    def _():
        for r in range(2):
            for j in range(GROUP):
                xr[r, GROUP - 1 + j] = zero_tile

    @pl.when(jnp.logical_not(has_prev))
    def _():
        for r in range(2):
            for j in range(GROUP):
                xr[r, 2 * GROUP - 1 + j] = zero_tile

    iy = lax.broadcasted_iota(jnp.int32, (ny, nz), 0)
    iz = lax.broadcasted_iota(jnp.int32, (ny, nz), 1)
    bottom_cell = iz == 0
    top_cell = iz == nz - 1
    low_mask = has_low.astype(F32)
    prev_mask = has_prev.astype(F32)
    next_mask = has_next.astype(F32)

    loads[0].wait()
    loads[1].wait()
    loads[2].wait()
    loads[3].wait()
    loads[4].start()
    loads[5].start()

    def x_face(l):
        return tx[0] * low_mask if l == 0 else tx[l]

    def raw(l):
        cy = jnp.where(iy > 0, ty[l], 0.0)
        tzl = tz[l]
        cz = jnp.where(bottom_cell, 0.0, tzl)
        dirichlet = jnp.where(bottom_cell, tzl * prev_mask, 0.0) + jnp.where(top_cell, tzl * next_mask, 0.0)
        cyu = roll(cy, -1, 0)
        czu = roll(cz, -1, 1)
        return cy, cyu, cz, czu, dirichlet

    def keep(l, w, parts, low, up):
        cy, cyu, cz, czu, dirichlet = parts
        ayd[l] = w * cy
        ayu[l] = w * cyu
        azd[l] = w * cz
        azu[l] = w * czu
        if l == 0:
            axh[0] = w * low
        else:
            axd[l] = w * low
        if l == top:
            axh[1] = w * up
        else:
            axu[l] = w * up
        b = w * src[l]
        bias[l] = b
        press[0, l] = b

    parts3 = raw(top)
    d3[...] = x_face(top) + parts3[0] + parts3[1] + parts3[2] + parts3[3] + parts3[4]

    def keep_low(l):
        parts = raw(l)
        low, up = x_face(l), tx[l + 1]
        diag = low + up + parts[0] + parts[1] + parts[2] + parts[3] + parts[4]
        keep(l, RELAX / diag, parts, low, up)

    keep_low(0)

    thin_row = lax.broadcasted_iota(jnp.int32, (8, ny), 0)
    thin_y = lax.broadcasted_iota(jnp.int32, (8, ny), 1)

    def thinned(layer):
        turned = layer.T
        return jnp.where(thin_row < 4, turned[0:8], turned[nz - 8 : nz])

    for l in range(layers):
        for f, ref in enumerate((tx, ty, tz, src)):
            value = thinned(ref[l])
            thin[l, f] = value * low_mask if l == 0 and f == 0 else value

    pl.semaphore_wait(barrier, greeted)

    def on_sides(act):
        @pl.when(has_low)
        def _():
            act(0)

        @pl.when(has_up)
        def _():
            act(1)

    def side_copy(side, source_ref, dest_ref, send_sem, recv_sem):
        return pltpu.make_async_remote_copy(
            src_ref=source_ref, dst_ref=dest_ref, send_sem=send_sem, recv_sem=recv_sem,
            device_id={"block": blk, "sub": sub - 1 + 2 * side}, device_id_type=MESH,
        )

    def thin_copies(side):
        if side == 0:
            return (
                side_copy(0, thin.at[0:2], thin_up.at[0:2], t_send.at[0], t_recv.at[0]),
                side_copy(0, thin.at[2, 0], thin_up.at[2, 0], t_send.at[1], t_recv.at[1]),
            )
        return (side_copy(1, thin.at[layers - 2 : layers], thin_low, t_send.at[2], t_recv.at[2]),)

    def near_copy(side):
        if side == 0:
            return side_copy(0, near.at[0:3], near_up, n_send.at[0], n_recv.at[0])
        return side_copy(1, near.at[layers - 3 : layers], near_low, n_send.at[1], n_recv.at[1])

    def g_copy(side):
        return side_copy(side, g_own, g_halo.at[1 - side], g_send.at[side], g_recv.at[1 - side])

    def start_all(copies):
        for copy in copies:
            copy.start()

    on_sides(lambda side: start_all(thin_copies(side)))

    def on_groups(act):
        @pl.when(group_low)
        def _():
            act(0)

        @pl.when(group_up)
        def _():
            act(1)

    def say_hello(r):
        def one(side):
            pl.semaphore_signal(
                hello.at[r, 1 - side], inc=1, device_id={"block": blk, "sub": sub - GROUP + 2 * GROUP * side},
                device_id_type=MESH,
            )

        if r < zgroups - 2:
            on_groups(one)

    def hear_hello(r):
        if r < zgroups - 2:
            on_groups(lambda side: pl.semaphore_wait(hello.at[r, side], 1))


    def e1_copy(i, rows=None):
        source_ref, dest_ref, step = (
            (tx.at[0], e1a.at[1], -1),
            (press.at[0, 0], e1b.at[1], -1),
            (d3, e1b.at[0], 1),
            (src.at[top], e1a.at[0], 1),
        )[i]
        if rows is not None:
            source_ref, dest_ref = source_ref.at[rows], dest_ref.at[rows]
        return pltpu.make_async_remote_copy(
            src_ref=source_ref, dst_ref=dest_ref, send_sem=e1_send.at[i], recv_sem=e1_recv.at[i],
            device_id={"block": blk, "sub": sub + step}, device_id_type=MESH,
        )

    def e1_part(i, c):
        source_ref = (tx.at[0], press.at[0, 0], d3, src.at[top])[i]
        helper = (xi + c) % GROUP if i >= 2 else (xi + GROUP - c) % GROUP
        return pltpu.make_async_remote_copy(
            src_ref=source_ref.at[quarter(c)], dst_ref=part1.at[i],
            send_sem=e1_send.at[i], recv_sem=p1_recv.at[i],
            device_id={"block": blk, "sub": zi * GROUP + helper}, device_id_type=MESH,
        )

    def e1_forward(i):
        dest_ref = (e1a.at[1], e1b.at[1], e1b.at[0], e1a.at[0])[i]
        if i >= 2:
            c, target = (xi + 1) % GROUP, (zi + 1) * GROUP
        else:
            c, target = (GROUP - xi) % GROUP, (zi - 1) * GROUP + GROUP - 1
        return pltpu.make_async_remote_copy(
            src_ref=part1.at[i], dst_ref=dest_ref.at[pl.ds(pl.multiple_of(8 + (c - 1) * rows_q, 8), rows_q)],
            send_sem=f1_send.at[i], recv_sem=e1_recv.at[i],
            device_id={"block": blk, "sub": target}, device_id_type=MESH,
        )

    helps_low = jnp.logical_not(first_x) & group_low
    helps_up = jnp.logical_not(last_x) & group_up

    for across, pair in ((slow_low, (0, 1)), (slow_up, (2, 3))):

        @pl.when(across)
        def _():
            for c in (2, 1, 3):
                for i in pair:
                    e1_part(i, c).start()
            for i in pair:
                e1_copy(i, pl.ds(0, 8)).start()

    for beside, pair in ((jnp.logical_not(first_x), (0, 1)), (jnp.logical_not(last_x), (2, 3))):

        @pl.when(beside)
        def _():
            for i in pair:
                e1_copy(i).start()

    for l in range(1, top):
        keep_low(l)

    for helps, pair in ((helps_low, (0, 1)), (helps_up, (2, 3))):

        @pl.when(helps)
        def _():
            for i in pair:
                e1_part(i, 1).wait_recv()
                e1_forward(i).start()

    def own_terms(k, l):
        p = press[k, l]
        return (
            (1.0 - RELAX) * p + bias[l]
            + ayd[l] * roll(p, 1, 0) + ayu[l] * roll(p, -1, 0)
            + azd[l] * roll(p, 1, 1) + azu[l] * roll(p, -1, 1)
        )

    def inner_layer(k, l):
        press[k + 1, l] = own_terms(k, l) + axd[l] * press[k, l - 1] + axu[l] * press[k, l + 1]

    def edge_terms(k, side):
        if side == 0:
            pre[0] = own_terms(k, 0) + axu[0] * press[k, 1]
        else:
            pre[1] = own_terms(k, top) + axd[top] * press[k, top - 1]

    def halo_copy(k, side, c):
        rows = pl.ds(c * rows_c, rows_c)
        return pltpu.make_async_remote_copy(
            src_ref=press.at[k, top * side, rows], dst_ref=halo.at[k - 1, 1 - side, rows],
            send_sem=h_send.at[k - 1, side, c], recv_sem=h_recv.at[k - 1, 1 - side, c],
            device_id={"block": blk, "sub": sub - 1 + 2 * side}, device_id_type=MESH,
        )

    def part_copy(k, side):
        return pltpu.make_async_remote_copy(
            src_ref=press.at[k, top * side, pl.ds(RELAYED[k] * rows_c, rows_c)], dst_ref=part.at[k - 1],
            send_sem=h_send.at[k - 1, side, RELAYED[k]], recv_sem=p_recv.at[k - 1],
            device_id={"block": blk, "sub": sub + 1 - 2 * side}, device_id_type=MESH,
        )

    help_side = (xi == GROUP - 2).astype(jnp.int32)
    helps = ((xi == GROUP - 2) & group_up) | ((xi == 1) & group_low)

    def forward_copy(k):
        return pltpu.make_async_remote_copy(
            src_ref=part.at[k - 1],
            dst_ref=halo.at[k - 1, 1 - help_side, pl.ds(RELAYED[k] * rows_c, rows_c)],
            send_sem=f_send.at[k - 1], recv_sem=h_recv.at[k - 1, 1 - help_side, RELAYED[k]],
            device_id={"block": blk, "sub": (zi - 1 + 2 * help_side) * GROUP + (1 - help_side) * (GROUP - 1)},
            device_id_type=MESH,
        )

    def forward(k):
        if RELAYED[k] is None:
            return

        @pl.when(helps)
        def _():
            part_copy(k, help_side).wait_recv()
            forward_copy(k).start()

    def has(side):
        return jnp.where(side == 0, has_low.astype(jnp.int32), has_up.astype(jnp.int32)) > 0

    def slow(side):
        return jnp.where(side == 0, first_x.astype(jnp.int32), last_x.astype(jnp.int32)) > 0

    def send_chunk(k, side, c):
        if c != RELAYED[k]:

            @pl.when(has(side))
            def _():
                halo_copy(k, side, c).start()

        else:

            @pl.when(has(side) & jnp.logical_not(slow(side)))
            def _():
                halo_copy(k, side, c).start()

            @pl.when(has(side) & slow(side))
            def _():
                part_copy(k, side).start()

    def send_side(k, side):
        for c in sorted(range(CHUNKS), key=lambda c: c != RELAYED[k]):
            send_chunk(k, side, c)

    first_side = jnp.logical_not(last_x).astype(jnp.int32)

    def edges(k, send):
        for t in range(2):
            side = first_side if t == 0 else 1 - first_side
            for c in sorted(range(CHUNKS), key=lambda c: c == RELAYED[k]):
                rows = pl.ds(c * rows_c, rows_c)

                @pl.when(has(side))
                def _():
                    halo_copy(k, 1 - side, c).wait_recv()

                press[k + 1, top * side, rows] = pre[side, rows] + axh[side, rows] * halo[k - 1, side, rows]
                if send:
                    send_chunk(k + 1, side, c)

    def x_copy(r, i):
        if i < GROUP - 1:
            target = {"block": blk, "sub": xpeer(i + 1)}
        elif i < 2 * GROUP - 1:
            target = {"block": blk - 1, "sub": xpeer(i - GROUP + 1)}
        else:
            target = {"block": blk + 1, "sub": xpeer(i - 2 * GROUP + 1)}
        return pltpu.make_async_remote_copy(
            src_ref=cbuf.at[r], dst_ref=xr.at[r, i], send_sem=x_send.at[r, i], recv_sem=x_recv.at[r, i],
            device_id=target, device_id_type=MESH,
        )

    own = range(GROUP - 1)
    low_block = range(GROUP - 1, 2 * GROUP - 1)
    up_block = range(2 * GROUP - 1, 3 * GROUP - 1)

    def x_start(r, acc):
        c_top, c_bot = (jnp.sum(v, axis=0, keepdims=True) for v in acc)
        for i in range(rows_m):
            cbuf[r, i : i + 1, :] = c_top[:, 128 * i : 128 * i + 128]
            cbuf[r, rows_m + i : rows_m + i + 1, :] = c_bot[:, 128 * i : 128 * i + 128]

        @pl.when(has_prev)
        def _():
            for i in low_block:
                x_copy(r, i).start()

        @pl.when(has_next)
        def _():
            for i in up_block:
                x_copy(r, i).start()

        for i in own:
            x_copy(r, i).start()

    def x_finish(r):
        for i in own:
            x_copy(r, i).wait_recv()

        @pl.when(has_next)
        def _():
            for i in low_block:
                x_copy(r, i).wait_recv()

        @pl.when(has_prev)
        def _():
            for i in up_block:
                x_copy(r, i).wait_recv()

        mine = cbuf[r]
        for i in own:
            mine = mine + xr[r, i]
        above = xr[r, low_block[0]]
        for i in low_block[1:]:
            above = above + xr[r, i]
        below = xr[r, up_block[0]]
        for i in up_block[1:]:
            below = below + xr[r, i]
        zs[r, 0:rows_m, :] = mine[0:rows_m] + above[rows_m : 2 * rows_m]
        zs[r, rows_m : 2 * rows_m, :] = below[0:rows_m] + mine[rows_m : 2 * rows_m]

    def z_copy(r, j):
        return pltpu.make_async_remote_copy(
            src_ref=zs.at[r], dst_ref=zr.at[r, j - 1], send_sem=z_send.at[r, j - 1], recv_sem=z_recv.at[r, j - 1],
            device_id={"block": blk, "sub": (zi + j) % zgroups * GROUP + xi}, device_id_type=MESH,
        )

    def z_start(r):
        for j in range(1, zgroups):
            z_copy(r, j).start()

    def z_finish(r):
        total = zs[r]
        for j in range(1, zgroups):
            z_copy(r, j).wait_recv()
            total = total + zr[r, j - 1]
        return MORTAR_STEP * total

    def project(fluxes):
        flat = jnp.concatenate([fluxes, jnp.zeros((128 - 2 * layers, ny), F32)], axis=0).T
        acc_t = jnp.zeros((8, mort), F32)
        acc_b = jnp.zeros((8, mort), F32)
        for l in range(layers):
            fb = flat[:, l : l + 1]
            ft = flat[:, layers + l : layers + l + 1]
            acc_b = acc_b + jnp.sum((fb * mb[l]).reshape(ny // 8, 8, mort), axis=0)
            acc_t = acc_t + jnp.sum((ft * mt[l]).reshape(ny // 8, 8, mort), axis=0)
        return acc_t, acc_b

    def face_rows(tiles):
        out = zero_thin
        for l in range(layers):
            out = jnp.where(thin_row == l, tiles[l][0:1, :], out)
            out = jnp.where(thin_row == layers + l, tiles[l][7:8, :], out)
        return out

    def thin_at(j, f):
        if j < 0:
            return thin_low[j + 2, f]
        return thin[j, f] if j < layers else thin_up[j - layers, f]

    def thin_terms(j):
        low, up = thin_at(j, 0), thin_at(j + 1, 0)
        cy = jnp.where(thin_y > 0, thin_at(j, 1), 0.0)
        tzj = thin_at(j, 2)
        cz = jnp.where(thin_row > 0, tzj, 0.0)
        cyu = roll(cy, -1, 1)
        czu = roll(cz, -1, 0)
        dirichlet = jnp.where(thin_row == 0, tzj * prev_mask, 0.0) + jnp.where(thin_row == 7, tzj * next_mask, 0.0)
        w = RELAX / (low + up + cy + cyu + cz + czu + dirichlet)
        return w, low, up, cy, cyu, cz, czu, dirichlet

    def thin_pass(terms, v, j, rhs):
        w, low, up, cy, cyu, cz, czu, _ = terms[j]
        d = v[j]
        return (1.0 - RELAX) * d + w * (
            rhs + low * v[j - 1] + up * v[j + 1]
            + cy * roll(d, 1, 1) + cyu * roll(d, -1, 1) + cz * roll(d, 1, 0) + czu * roll(d, -1, 0)
        )

    def low_edge():
        @pl.when(has_low)
        def _():
            e1_copy(2).wait_recv()
            e1_copy(3).wait_recv()

        press[1, 0] = pre[0] + axh[0] * (RELAX * e1a[0] / (e1b[0] + x_face(0)))
        send_side(1, 0)

    def up_edge():
        @pl.when(has_up)
        def _():
            e1_copy(0).wait_recv()

        x_up = e1a[1]
        keep(top, RELAX / (d3[...] + x_up), raw(top), x_face(top), x_up)
        edge_terms(0, 1)

        @pl.when(has_up)
        def _():
            e1_copy(1).wait_recv()

        press[1, top] = pre[1] + axh[1] * e1b[1]
        send_side(1, 1)

    inner_layer(0, 1)
    edge_terms(0, 0)

    @pl.when(last_x)
    def _():
        low_edge()

    @pl.when(first_x)
    def _():
        up_edge()

    say_hello(0)

    loads[4].wait()
    loads[5].wait()

    def wait_all(copies):
        for copy in copies:
            copy.wait_recv()

    on_sides(lambda side: wait_all(thin_copies(1 - side)))
    terms = {j: thin_terms(j) for j in range(-2, layers + 2)}
    level = {j: terms[j][0] * thin_at(j, 3) for j in terms}
    level = {j: thin_pass(terms, level, j, thin_at(j, 3)) for j in range(-1, layers + 1)}
    level = {j: thin_pass(terms, level, j, thin_at(j, 3)) for j in range(layers)}
    x_start(0, project(face_rows({l: terms[l][7] * level[l] for l in range(layers)})))

    @pl.when(jnp.logical_not(first_x))
    def _():
        up_edge()

    @pl.when(jnp.logical_not(last_x))
    def _():
        low_edge()

    inner_layer(0, top - 1)
    for r in range(zgroups - 2):
        hear_hello(r)
        say_hello(r + 1)
    x_finish(0)
    z_start(0)
    forward(1)

    def one_pass(k, send):
        for l in range(1, top):
            inner_layer(k, l)
        edge_terms(k, 0)
        edge_terms(k, 1)
        edges(k, send)

    one_pass(1, True)
    for l in range(layers):
        near[l] = thinned(press[2, l])
    on_sides(lambda side: near_copy(side).start())
    for l in range(1, top):
        inner_layer(2, l)
    edge_terms(2, 0)
    edge_terms(2, 1)
    forward(2)
    mortar = z_finish(0)
    here = jnp.concatenate([mortar[i : i + 1, :] for i in range(rows_m)], axis=1)
    under = jnp.concatenate([mortar[rows_m + i : rows_m + i + 1, :] for i in range(rows_m)], axis=1)

    columns = zero_layer
    for l in range(layers):
        gb = jnp.sum(mb[l] * under, axis=1, keepdims=True)
        gt = jnp.sum(mt[l] * here, axis=1, keepdims=True)
        columns = jnp.where(iz == l, gb, columns)
        columns = jnp.where(iz == layers + l, gt, columns)
    g_own[...] = columns.T[0 : 2 * layers]
    on_sides(lambda side: g_copy(side).start())

    early = zi < 2

    @pl.when(early)
    def _():
        edges(2, True)


    on_sides(lambda side: near_copy(1 - side).wait_recv())
    terms = {j: thin_terms(j) for j in range(-2, layers + 2)}
    level = {j: near_low[j + 3] if j < 0 else near[j] if j < layers else near_up[j - layers] for j in range(-3, layers + 3)}
    for width in (2, 1, 0):
        level = {j: thin_pass(terms, level, j, thin_at(j, 3)) for j in range(-width, layers + width)}

    on_sides(lambda side: g_copy(1 - side).wait_recv())

    def g_at(j):
        i = j % layers
        ref = g_halo.at[0] if j < 0 else g_own if j < layers else g_halo.at[1]
        return jnp.where(thin_row < 4, ref[i : i + 1, :], ref[layers + i : layers + i + 1, :])

    given = {j: terms[j][7] * g_at(j) for j in terms}
    extra = {j: terms[j][0] * given[j] for j in terms}
    for width in (1, 0):
        extra = {j: thin_pass(terms, extra, j, given[j]) for j in range(-width, layers + width)}
    x_start(1, project(face_rows({l: terms[l][7] * (level[l] + extra[l] - g_at(l)) for l in range(layers)})))

    def added(l):
        d = extra[l]
        tall = jnp.concatenate(
            [jnp.where(thin_row < 4, d, 0.0), jnp.zeros((nz - 16, ny), F32), jnp.where(thin_row < 4, 0.0, d)], axis=0
        )
        return tall.T

    for l in range(layers):
        grid_d[l] = added(l)

    @pl.when(jnp.logical_not(early))
    def _():
        edges(2, True)

    for l in range(1, top):
        inner_layer(3, l)
    edge_terms(3, 0)
    edge_terms(3, 1)
    forward(3)
    x_finish(1)
    z_start(1)
    edges(3, True)
    forward(4)
    for l in range(1, top):
        inner_layer(4, l)
    edge_terms(4, 0)
    edge_terms(4, 1)
    for l in range(1, top):
        p_out[0, l] = press[5, l] + grid_d[l]
    edges(4, False)
    for l in (0, top):
        p_out[0, l] = press[5, l] + grid_d[l]
    final = mortar + z_finish(1)
    share = mort // sub_count
    offset = sub * share
    row = final[0:1, :]
    for i in range(1, rows_m):
        row = jnp.where(offset // 128 == i, final[i : i + 1, :], row)
    wide = jnp.broadcast_to(row, (8, 128))
    m_out[...] = pltpu.roll(wide, (128 - offset % 128) % 128, 1)[0:1, 0:share]

    def sent_all(copies):
        for copy in copies:
            copy.wait_send()

    on_sides(lambda side: sent_all(thin_copies(side)))
    on_sides(lambda side: near_copy(side).wait_send())
    on_sides(lambda side: g_copy(side).wait_send())

    @pl.when(has_low)
    def _():
        e1_copy(0).wait_send()
        e1_copy(1).wait_send()
        for k in range(1, 5):
            for c in range(CHUNKS):
                halo_copy(k, 0, c).wait_send()

    @pl.when(has_up)
    def _():
        e1_copy(2).wait_send()
        e1_copy(3).wait_send()
        for k in range(1, 5):
            for c in range(CHUNKS):
                halo_copy(k, 1, c).wait_send()

    @pl.when(helps_low)
    def _():
        e1_forward(0).wait_send()
        e1_forward(1).wait_send()

    @pl.when(helps_up)
    def _():
        e1_forward(2).wait_send()
        e1_forward(3).wait_send()

    @pl.when(helps)
    def _():
        for k in range(1, 5):
            if RELAYED[k] is not None:
                forward_copy(k).wait_send()

    for r in range(2):
        for i in own:
            x_copy(r, i).wait_send()
        for j in range(1, zgroups):
            z_copy(r, j).wait_send()

    @pl.when(has_prev)
    def _():
        for r in range(2):
            for i in low_block:
                x_copy(r, i).wait_send()

    @pl.when(has_next)
    def _():
        for r in range(2):
            for i in up_block:
                x_copy(r, i).wait_send()


def shards(source, trans_x, trans_y, trans_z, mortar_bot, mortar_top):
    _, layers, ny, nz = source.shape
    mort = mortar_bot.shape[3]
    sub_count = lax.axis_size("sub")
    block_count = lax.axis_size("block")
    zgroups = sub_count // GROUP
    field = pltpu.VMEM((layers, ny, nz), F32)
    basis = pltpu.VMEM((layers, ny, mort), F32)
    pair = pltpu.VMEM((2, ny, nz), F32)
    dma = pltpu.SemaphoreType.DMA
    xmsgs = 3 * GROUP - 1
    hbm = pl.BlockSpec(memory_space=pl.ANY)
    vmem = pl.BlockSpec(memory_space=pltpu.VMEM)
    return pl.pallas_call(
        functools.partial(kernel, sub_count, block_count),
        out_shape=(
            pltpu.VMEM(source.shape, F32),
            pltpu.VMEM((1, mort // sub_count), F32),
        ),
        in_specs=[hbm] * 6,
        out_specs=(vmem, vmem),
        scratch_shapes=[
            field, field, field, field, basis, basis,
            field, field, field, field, field, field, pair, field,
            pltpu.VMEM((6, layers, ny, nz), F32), pair, field,
            pltpu.VMEM((ny, nz), F32), pair, pair, pltpu.VMEM((4, 2, ny, nz), F32),
            pltpu.VMEM((2, 8, 128), F32), pltpu.VMEM((2, xmsgs, 8, 128), F32),
            pltpu.VMEM((2, 8, 128), F32), pltpu.VMEM((2, zgroups - 1, 8, 128), F32),
            pltpu.VMEM((4, (ny - 8) // (GROUP - 1), nz), F32), pltpu.VMEM((4, ny // CHUNKS, nz), F32),
            pltpu.VMEM((layers, 4, 8, ny), F32), pltpu.VMEM((2, 4, 8, ny), F32), pltpu.VMEM((3, 4, 8, ny), F32),
            pltpu.VMEM((layers, 8, ny), F32), pltpu.VMEM((3, 8, ny), F32), pltpu.VMEM((3, 8, ny), F32),
            pltpu.VMEM((2 * layers, ny), F32), pltpu.VMEM((2, 2 * layers, ny), F32),
            dma((6,)), dma((4,)), dma((4,)),
            dma((4, 2, CHUNKS)), dma((4, 2, CHUNKS)),
            dma((2, xmsgs)), dma((2, xmsgs)), dma((2, zgroups - 1)), dma((2, zgroups - 1)),
            dma((4,)), dma((4,)), dma((4,)), dma((4,)),
            dma((3,)), dma((3,)), dma((2,)), dma((2,)), dma((2,)), dma((2,)),
            pltpu.SemaphoreType.REGULAR((max(zgroups - 2, 1), 2)),
        ],
        compiler_params=pltpu.CompilerParams(collective_id=0, has_side_effects=True),
        name="mortar_darcy",
    )(source, trans_x, trans_y, trans_z, mortar_bot, mortar_top)


def solution(mesh):
    spec = P("block", "sub", None, None)
    return jax.shard_map(
        shards,
        mesh=mesh,
        in_specs=(spec,) * 6,
        out_specs=(spec, P("block", "sub")),
        check_vma=False,
    )
```

```python
import functools
import jax
import jax.numpy as jnp
from jax import lax
from jax.experimental import pallas as pl
from jax.experimental.pallas import tpu as pltpu
from jax.sharding import PartitionSpec as P

RELAX = 0.8
MORTAR_STEP = 0.05
MESH = pl.DeviceIdType.MESH
GROUP = 4
CHUNKS = 4
RELAYED = {1: 3, 2: 0, 3: 3, 4: 0}
F32 = jnp.float32


def roll(value, shift, axis):
    return pltpu.roll(value, shift % value.shape[axis], axis)


def kernel(
    sub_count, block_count,
    src_h, tx_h, ty_h, tz_h, mb_h, mt_h, p_out, m_out,
    src, tx, ty, tz, mb, mt,
    ayd, ayu, azd, azu, axd, axu, axh, bias, press, pre, grid_d,
    d3, e1a, e1b, halo, cbuf, xr, zs, zr, part1, part, thin, thin_low, thin_up, near, near_low, near_up, g_own, g_halo,
    load_sem, e1_send, e1_recv, h_send, h_recv, x_send, x_recv, z_send, z_recv,
    p1_recv, f1_send, p_recv, f_send, t_send, t_recv, n_send, n_recv, g_send, g_recv, hello,
):
    layers, ny, nz = src.shape
    top = layers - 1
    mort = mb.shape[2]
    rows_m = mort // 128
    sub = lax.axis_index("sub")
    blk = lax.axis_index("block")
    xi = sub % GROUP
    zi = sub // GROUP
    zgroups = sub_count // GROUP
    has_low = sub > 0
    has_up = sub < sub_count - 1
    has_prev = blk > 0
    has_next = blk < block_count - 1
    rows_c = ny // CHUNKS
    rows_q = (ny - 8) // (GROUP - 1)

    def quarter(c):
        return pl.ds(8 + (c - 1) * rows_q, rows_q)

    first_x = xi == 0
    last_x = xi == GROUP - 1
    group_low = zi > 0
    group_up = zi < zgroups - 1
    inside_x = jnp.logical_not(first_x | last_x)

    loads = []
    for i, (h, v) in enumerate(((tx_h, tx), (ty_h, ty), (tz_h, tz), (src_h, src), (mb_h, mb), (mt_h, mt))):
        cp = pltpu.make_async_copy(h.at[0], v, load_sem.at[i])
        loads.append(cp)
        if i < 4:
            cp.start()

    barrier = pltpu.get_barrier_semaphore()

    def greet(b, s):
        pl.semaphore_signal(barrier, inc=1, device_id={"block": b, "sub": s}, device_id_type=MESH)

    def xpeer(j):
        return zi * GROUP + (xi + j) % GROUP

    slow_low = first_x & group_low
    slow_up = last_x & group_up
    pass_low = inside_x & group_low
    pass_up = inside_x & group_up

    @pl.when(slow_low)
    def _():
        for j in range(1, GROUP):
            greet(blk, sub - j)

    @pl.when(slow_up)
    def _():
        for j in range(1, GROUP):
            greet(blk, sub + j)

    @pl.when(pass_low)
    def _():
        greet(blk, (zi - 1) * GROUP + GROUP - 1)

    @pl.when(pass_up)
    def _():
        greet(blk, (zi + 1) * GROUP)

    for j in range(1, GROUP):
        greet(blk, xpeer(j))

    @pl.when(group_low & jnp.logical_not(first_x))
    def _():
        greet(blk, sub - GROUP)

    @pl.when(group_up)
    def _():
        greet(blk, sub + GROUP)

    @pl.when(has_prev)
    def _():
        for j in range(GROUP):
            greet(blk - 1, xpeer(j))

    @pl.when(has_next)
    def _():
        for j in range(GROUP):
            greet(blk + 1, xpeer(j))

    greeted = (
        GROUP - 1 + group_low.astype(jnp.int32) + (group_up & jnp.logical_not(first_x)).astype(jnp.int32)
        + (GROUP - 1) * (slow_low.astype(jnp.int32) + slow_up.astype(jnp.int32))
        + pass_low.astype(jnp.int32) + pass_up.astype(jnp.int32)
        + GROUP * has_prev.astype(jnp.int32) + GROUP * has_next.astype(jnp.int32)
    )

    zero_layer = jnp.zeros((ny, nz), F32)
    zero_thin = jnp.zeros((8, ny), F32)

    @pl.when(jnp.logical_not(has_low))
    def _():
        e1a[0] = zero_layer
        e1b[0] = zero_layer + 1.0
        for e in range(4):
            halo[e, 0] = zero_layer
        g_halo[0] = zero_thin
        for i in range(2):
            for f in range(4):
                thin_low[i, f] = zero_thin + (0.0 if f == 3 else 1.0)
        for i in range(3):
            near_low[i] = zero_thin

    @pl.when(jnp.logical_not(has_up))
    def _():
        e1a[1] = zero_layer
        e1b[1] = zero_layer
        for e in range(4):
            halo[e, 1] = zero_layer
        g_halo[1] = zero_thin
        for i in range(3):
            for f in range(4):
                thin_up[i, f] = zero_thin + (0.0 if f == 3 or (i == 0 and f == 0) else 1.0)
        for i in range(3):
            near_up[i] = zero_thin

    zero_tile = jnp.zeros((8, 128), F32)
    for r in range(2):
        cbuf[r] = zero_tile
        zs[r] = zero_tile

    @pl.when(jnp.logical_not(has_next))
    def _():
        for r in range(2):
            for j in range(GROUP):
                xr[r, GROUP - 1 + j] = zero_tile

    @pl.when(jnp.logical_not(has_prev))
    def _():
        for r in range(2):
            for j in range(GROUP):
                xr[r, 2 * GROUP - 1 + j] = zero_tile

    iy = lax.broadcasted_iota(jnp.int32, (ny, nz), 0)
    iz = lax.broadcasted_iota(jnp.int32, (ny, nz), 1)
    bottom_cell = iz == 0
    top_cell = iz == nz - 1
    low_mask = has_low.astype(F32)
    prev_mask = has_prev.astype(F32)
    next_mask = has_next.astype(F32)

    loads[0].wait()
    loads[1].wait()
    loads[2].wait()
    loads[3].wait()
    loads[4].start()
    loads[5].start()

    def x_face(l):
        return tx[0] * low_mask if l == 0 else tx[l]

    def raw(l):
        cy = jnp.where(iy > 0, ty[l], 0.0)
        tzl = tz[l]
        cz = jnp.where(bottom_cell, 0.0, tzl)
        dirichlet = jnp.where(bottom_cell, tzl * prev_mask, 0.0) + jnp.where(top_cell, tzl * next_mask, 0.0)
        cyu = roll(cy, -1, 0)
        czu = roll(cz, -1, 1)
        return cy, cyu, cz, czu, dirichlet

    def keep(l, w, parts, low, up):
        cy, cyu, cz, czu, dirichlet = parts
        ayd[l] = w * cy
        ayu[l] = w * cyu
        azd[l] = w * cz
        azu[l] = w * czu
        if l == 0:
            axh[0] = w * low
        else:
            axd[l] = w * low
        if l == top:
            axh[1] = w * up
        else:
            axu[l] = w * up
        b = w * src[l]
        bias[l] = b
        press[0, l] = b

    parts3 = raw(top)
    d3[...] = x_face(top) + parts3[0] + parts3[1] + parts3[2] + parts3[3] + parts3[4]

    def keep_low(l):
        parts = raw(l)
        low, up = x_face(l), tx[l + 1]
        diag = low + up + parts[0] + parts[1] + parts[2] + parts[3] + parts[4]
        keep(l, RELAX / diag, parts, low, up)

    keep_low(0)

    thin_row = lax.broadcasted_iota(jnp.int32, (8, ny), 0)
    thin_y = lax.broadcasted_iota(jnp.int32, (8, ny), 1)

    def thinned(layer):
        turned = layer.T
        return jnp.where(thin_row < 4, turned[0:8], turned[nz - 8 : nz])

    for l in range(layers):
        for f, ref in enumerate((tx, ty, tz, src)):
            value = thinned(ref[l])
            thin[l, f] = value * low_mask if l == 0 and f == 0 else value

    pl.semaphore_wait(barrier, greeted)

    def on_sides(act):
        @pl.when(has_low)
        def _():
            act(0)

        @pl.when(has_up)
        def _():
            act(1)

    def side_copy(side, source_ref, dest_ref, send_sem, recv_sem):
        return pltpu.make_async_remote_copy(
            src_ref=source_ref, dst_ref=dest_ref, send_sem=send_sem, recv_sem=recv_sem,
            device_id={"block": blk, "sub": sub - 1 + 2 * side}, device_id_type=MESH,
        )

    def thin_copies(side):
        if side == 0:
            return (
                side_copy(0, thin.at[0:2], thin_up.at[0:2], t_send.at[0], t_recv.at[0]),
                side_copy(0, thin.at[2, 0], thin_up.at[2, 0], t_send.at[1], t_recv.at[1]),
            )
        return (side_copy(1, thin.at[layers - 2 : layers], thin_low, t_send.at[2], t_recv.at[2]),)

    def near_copy(side):
        if side == 0:
            return side_copy(0, near.at[0:3], near_up, n_send.at[0], n_recv.at[0])
        return side_copy(1, near.at[layers - 3 : layers], near_low, n_send.at[1], n_recv.at[1])

    def g_copy(side):
        return side_copy(side, g_own, g_halo.at[1 - side], g_send.at[side], g_recv.at[1 - side])

    def start_all(copies):
        for copy in copies:
            copy.start()

    on_sides(lambda side: start_all(thin_copies(side)))

    def on_groups(act):
        @pl.when(group_low)
        def _():
            act(0)

        @pl.when(group_up)
        def _():
            act(1)

    def say_hello(r):
        def one(side):
            pl.semaphore_signal(
                hello.at[r, 1 - side], inc=1, device_id={"block": blk, "sub": sub - GROUP + 2 * GROUP * side},
                device_id_type=MESH,
            )

        if r < zgroups - 2:
            on_groups(one)

    def hear_hello(r):
        if r < zgroups - 2:
            on_groups(lambda side: pl.semaphore_wait(hello.at[r, side], 1))


    def e1_copy(i, rows=None):
        source_ref, dest_ref, step = (
            (tx.at[0], e1a.at[1], -1),
            (press.at[0, 0], e1b.at[1], -1),
            (d3, e1b.at[0], 1),
            (src.at[top], e1a.at[0], 1),
        )[i]
        if rows is not None:
            source_ref, dest_ref = source_ref.at[rows], dest_ref.at[rows]
        return pltpu.make_async_remote_copy(
            src_ref=source_ref, dst_ref=dest_ref, send_sem=e1_send.at[i], recv_sem=e1_recv.at[i],
            device_id={"block": blk, "sub": sub + step}, device_id_type=MESH,
        )

    def e1_part(i, c):
        source_ref = (tx.at[0], press.at[0, 0], d3, src.at[top])[i]
        helper = (xi + c) % GROUP if i >= 2 else (xi + GROUP - c) % GROUP
        return pltpu.make_async_remote_copy(
            src_ref=source_ref.at[quarter(c)], dst_ref=part1.at[i],
            send_sem=e1_send.at[i], recv_sem=p1_recv.at[i],
            device_id={"block": blk, "sub": zi * GROUP + helper}, device_id_type=MESH,
        )

    def e1_forward(i):
        dest_ref = (e1a.at[1], e1b.at[1], e1b.at[0], e1a.at[0])[i]
        if i >= 2:
            c, target = (xi + 1) % GROUP, (zi + 1) * GROUP
        else:
            c, target = (GROUP - xi) % GROUP, (zi - 1) * GROUP + GROUP - 1
        return pltpu.make_async_remote_copy(
            src_ref=part1.at[i], dst_ref=dest_ref.at[pl.ds(pl.multiple_of(8 + (c - 1) * rows_q, 8), rows_q)],
            send_sem=f1_send.at[i], recv_sem=e1_recv.at[i],
            device_id={"block": blk, "sub": target}, device_id_type=MESH,
        )

    helps_low = jnp.logical_not(first_x) & group_low
    helps_up = jnp.logical_not(last_x) & group_up

    for across, pair in ((slow_low, (0, 1)), (slow_up, (2, 3))):

        @pl.when(across)
        def _():
            for c in (2, 1, 3):
                for i in pair:
                    e1_part(i, c).start()
            for i in pair:
                e1_copy(i, pl.ds(0, 8)).start()

    for beside, pair in ((jnp.logical_not(first_x), (0, 1)), (jnp.logical_not(last_x), (2, 3))):

        @pl.when(beside)
        def _():
            for i in pair:
                e1_copy(i).start()

    for l in range(1, top):
        keep_low(l)

    for helps, pair in ((helps_low, (0, 1)), (helps_up, (2, 3))):

        @pl.when(helps)
        def _():
            for i in pair:
                e1_part(i, 1).wait_recv()
                e1_forward(i).start()

    def own_terms(k, l):
        p = press[k, l]
        return (
            (1.0 - RELAX) * p + bias[l]
            + ayd[l] * roll(p, 1, 0) + ayu[l] * roll(p, -1, 0)
            + azd[l] * roll(p, 1, 1) + azu[l] * roll(p, -1, 1)
        )

    def inner_layer(k, l):
        press[k + 1, l] = own_terms(k, l) + axd[l] * press[k, l - 1] + axu[l] * press[k, l + 1]

    def edge_terms(k, side):
        if side == 0:
            pre[0] = own_terms(k, 0) + axu[0] * press[k, 1]
        else:
            pre[1] = own_terms(k, top) + axd[top] * press[k, top - 1]

    def halo_copy(k, side, c):
        rows = pl.ds(c * rows_c, rows_c)
        return pltpu.make_async_remote_copy(
            src_ref=press.at[k, top * side, rows], dst_ref=halo.at[k - 1, 1 - side, rows],
            send_sem=h_send.at[k - 1, side, c], recv_sem=h_recv.at[k - 1, 1 - side, c],
            device_id={"block": blk, "sub": sub - 1 + 2 * side}, device_id_type=MESH,
        )

    def part_copy(k, side):
        return pltpu.make_async_remote_copy(
            src_ref=press.at[k, top * side, pl.ds(RELAYED[k] * rows_c, rows_c)], dst_ref=part.at[k - 1],
            send_sem=h_send.at[k - 1, side, RELAYED[k]], recv_sem=p_recv.at[k - 1],
            device_id={"block": blk, "sub": sub + 1 - 2 * side}, device_id_type=MESH,
        )

    help_side = (xi == GROUP - 2).astype(jnp.int32)
    helps = ((xi == GROUP - 2) & group_up) | ((xi == 1) & group_low)

    def forward_copy(k):
        return pltpu.make_async_remote_copy(
            src_ref=part.at[k - 1],
            dst_ref=halo.at[k - 1, 1 - help_side, pl.ds(RELAYED[k] * rows_c, rows_c)],
            send_sem=f_send.at[k - 1], recv_sem=h_recv.at[k - 1, 1 - help_side, RELAYED[k]],
            device_id={"block": blk, "sub": (zi - 1 + 2 * help_side) * GROUP + (1 - help_side) * (GROUP - 1)},
            device_id_type=MESH,
        )

    def forward(k):
        if RELAYED[k] is None:
            return

        @pl.when(helps)
        def _():
            part_copy(k, help_side).wait_recv()
            forward_copy(k).start()

    def has(side):
        return jnp.where(side == 0, has_low.astype(jnp.int32), has_up.astype(jnp.int32)) > 0

    def slow(side):
        return jnp.where(side == 0, first_x.astype(jnp.int32), last_x.astype(jnp.int32)) > 0

    def send_chunk(k, side, c):
        if c != RELAYED[k]:

            @pl.when(has(side))
            def _():
                halo_copy(k, side, c).start()

        else:

            @pl.when(has(side) & jnp.logical_not(slow(side)))
            def _():
                halo_copy(k, side, c).start()

            @pl.when(has(side) & slow(side))
            def _():
                part_copy(k, side).start()

    def send_side(k, side):
        for c in sorted(range(CHUNKS), key=lambda c: c != RELAYED[k]):
            send_chunk(k, side, c)

    first_side = jnp.logical_not(last_x).astype(jnp.int32)

    def edges(k, send):
        for t in range(2):
            side = first_side if t == 0 else 1 - first_side
            for c in sorted(range(CHUNKS), key=lambda c: c == RELAYED[k]):
                rows = pl.ds(c * rows_c, rows_c)

                @pl.when(has(side))
                def _():
                    halo_copy(k, 1 - side, c).wait_recv()

                press[k + 1, top * side, rows] = pre[side, rows] + axh[side, rows] * halo[k - 1, side, rows]
                if send:
                    send_chunk(k + 1, side, c)

    def x_copy(r, i):
        if i < GROUP - 1:
            target = {"block": blk, "sub": xpeer(i + 1)}
        elif i < 2 * GROUP - 1:
            target = {"block": blk - 1, "sub": xpeer(i - GROUP + 1)}
        else:
            target = {"block": blk + 1, "sub": xpeer(i - 2 * GROUP + 1)}
        return pltpu.make_async_remote_copy(
            src_ref=cbuf.at[r], dst_ref=xr.at[r, i], send_sem=x_send.at[r, i], recv_sem=x_recv.at[r, i],
            device_id=target, device_id_type=MESH,
        )

    own = range(GROUP - 1)
    low_block = range(GROUP - 1, 2 * GROUP - 1)
    up_block = range(2 * GROUP - 1, 3 * GROUP - 1)

    def x_start(r, acc):
        c_top, c_bot = (jnp.sum(v, axis=0, keepdims=True) for v in acc)
        for i in range(rows_m):
            cbuf[r, i : i + 1, :] = c_top[:, 128 * i : 128 * i + 128]
            cbuf[r, rows_m + i : rows_m + i + 1, :] = c_bot[:, 128 * i : 128 * i + 128]

        @pl.when(has_prev)
        def _():
            for i in low_block:
                x_copy(r, i).start()

        @pl.when(has_next)
        def _():
            for i in up_block:
                x_copy(r, i).start()

        for i in own:
            x_copy(r, i).start()

    def x_finish(r):
        for i in own:
            x_copy(r, i).wait_recv()

        @pl.when(has_next)
        def _():
            for i in low_block:
                x_copy(r, i).wait_recv()

        @pl.when(has_prev)
        def _():
            for i in up_block:
                x_copy(r, i).wait_recv()

        mine = cbuf[r]
        for i in own:
            mine = mine + xr[r, i]
        above = xr[r, low_block[0]]
        for i in low_block[1:]:
            above = above + xr[r, i]
        below = xr[r, up_block[0]]
        for i in up_block[1:]:
            below = below + xr[r, i]
        zs[r, 0:rows_m, :] = mine[0:rows_m] + above[rows_m : 2 * rows_m]
        zs[r, rows_m : 2 * rows_m, :] = below[0:rows_m] + mine[rows_m : 2 * rows_m]

    def z_copy(r, j):
        return pltpu.make_async_remote_copy(
            src_ref=zs.at[r], dst_ref=zr.at[r, j - 1], send_sem=z_send.at[r, j - 1], recv_sem=z_recv.at[r, j - 1],
            device_id={"block": blk, "sub": (zi + j) % zgroups * GROUP + xi}, device_id_type=MESH,
        )

    def z_start(r):
        for j in range(1, zgroups):
            z_copy(r, j).start()

    def z_finish(r):
        total = zs[r]
        for j in range(1, zgroups):
            z_copy(r, j).wait_recv()
            total = total + zr[r, j - 1]
        return MORTAR_STEP * total

    def project(fluxes):
        flat = jnp.concatenate([fluxes, jnp.zeros((128 - 2 * layers, ny), F32)], axis=0).T
        acc_t = jnp.zeros((8, mort), F32)
        acc_b = jnp.zeros((8, mort), F32)
        for l in range(layers):
            fb = flat[:, l : l + 1]
            ft = flat[:, layers + l : layers + l + 1]
            acc_b = acc_b + jnp.sum((fb * mb[l]).reshape(ny // 8, 8, mort), axis=0)
            acc_t = acc_t + jnp.sum((ft * mt[l]).reshape(ny // 8, 8, mort), axis=0)
        return acc_t, acc_b

    def face_rows(tiles):
        out = zero_thin
        for l in range(layers):
            out = jnp.where(thin_row == l, tiles[l][0:1, :], out)
            out = jnp.where(thin_row == layers + l, tiles[l][7:8, :], out)
        return out

    def thin_at(j, f):
        if j < 0:
            return thin_low[j + 2, f]
        return thin[j, f] if j < layers else thin_up[j - layers, f]

    def thin_terms(j):
        low, up = thin_at(j, 0), thin_at(j + 1, 0)
        cy = jnp.where(thin_y > 0, thin_at(j, 1), 0.0)
        tzj = thin_at(j, 2)
        cz = jnp.where(thin_row > 0, tzj, 0.0)
        cyu = roll(cy, -1, 1)
        czu = roll(cz, -1, 0)
        dirichlet = jnp.where(thin_row == 0, tzj * prev_mask, 0.0) + jnp.where(thin_row == 7, tzj * next_mask, 0.0)
        w = RELAX / (low + up + cy + cyu + cz + czu + dirichlet)
        return w, low, up, cy, cyu, cz, czu, dirichlet

    def thin_pass(terms, v, j, rhs):
        w, low, up, cy, cyu, cz, czu, _ = terms[j]
        d = v[j]
        return (1.0 - RELAX) * d + w * (
            rhs + low * v[j - 1] + up * v[j + 1]
            + cy * roll(d, 1, 1) + cyu * roll(d, -1, 1) + cz * roll(d, 1, 0) + czu * roll(d, -1, 0)
        )

    def low_edge():
        @pl.when(has_low)
        def _():
            e1_copy(2).wait_recv()
            e1_copy(3).wait_recv()

        press[1, 0] = pre[0] + axh[0] * (RELAX * e1a[0] / (e1b[0] + x_face(0)))
        send_side(1, 0)

    def up_edge():
        @pl.when(has_up)
        def _():
            e1_copy(0).wait_recv()

        x_up = e1a[1]
        keep(top, RELAX / (d3[...] + x_up), raw(top), x_face(top), x_up)
        edge_terms(0, 1)

        @pl.when(has_up)
        def _():
            e1_copy(1).wait_recv()

        press[1, top] = pre[1] + axh[1] * e1b[1]
        send_side(1, 1)

    inner_layer(0, 1)
    edge_terms(0, 0)

    @pl.when(last_x)
    def _():
        low_edge()

    @pl.when(first_x)
    def _():
        up_edge()

    say_hello(0)

    loads[4].wait()
    loads[5].wait()

    def wait_all(copies):
        for copy in copies:
            copy.wait_recv()

    on_sides(lambda side: wait_all(thin_copies(1 - side)))
    for r in range(zgroups - 3):
        hear_hello(r)
        say_hello(r + 1)
    terms = {j: thin_terms(j) for j in range(-2, layers + 2)}
    level = {j: terms[j][0] * thin_at(j, 3) for j in terms}
    level = {j: thin_pass(terms, level, j, thin_at(j, 3)) for j in range(-1, layers + 1)}
    level = {j: thin_pass(terms, level, j, thin_at(j, 3)) for j in range(layers)}
    x_start(0, project(face_rows({l: terms[l][7] * level[l] for l in range(layers)})))

    @pl.when(jnp.logical_not(first_x))
    def _():
        up_edge()

    @pl.when(jnp.logical_not(last_x))
    def _():
        low_edge()

    inner_layer(0, top - 1)
    if zgroups > 2:
        hear_hello(zgroups - 3)
    x_finish(0)
    z_start(0)
    forward(1)

    def one_pass(k, send):
        for l in range(1, top):
            inner_layer(k, l)
        edge_terms(k, 0)
        edge_terms(k, 1)
        edges(k, send)

    one_pass(1, True)
    for l in range(layers):
        near[l] = thinned(press[2, l])
    on_sides(lambda side: near_copy(side).start())
    for l in range(1, top):
        inner_layer(2, l)
    edge_terms(2, 0)
    edge_terms(2, 1)
    forward(2)
    mortar = z_finish(0)
    here = jnp.concatenate([mortar[i : i + 1, :] for i in range(rows_m)], axis=1)
    under = jnp.concatenate([mortar[rows_m + i : rows_m + i + 1, :] for i in range(rows_m)], axis=1)

    columns = zero_layer
    for l in range(layers):
        gb = jnp.sum(mb[l] * under, axis=1, keepdims=True)
        gt = jnp.sum(mt[l] * here, axis=1, keepdims=True)
        columns = jnp.where(iz == l, gb, columns)
        columns = jnp.where(iz == layers + l, gt, columns)
    g_own[...] = columns.T[0 : 2 * layers]
    on_sides(lambda side: g_copy(side).start())

    early = zi < 2

    @pl.when(early)
    def _():
        edges(2, True)


    on_sides(lambda side: near_copy(1 - side).wait_recv())
    terms = {j: thin_terms(j) for j in range(-2, layers + 2)}
    level = {j: near_low[j + 3] if j < 0 else near[j] if j < layers else near_up[j - layers] for j in range(-3, layers + 3)}
    for width in (2, 1, 0):
        level = {j: thin_pass(terms, level, j, thin_at(j, 3)) for j in range(-width, layers + width)}

    on_sides(lambda side: g_copy(1 - side).wait_recv())

    def g_at(j):
        i = j % layers
        ref = g_halo.at[0] if j < 0 else g_own if j < layers else g_halo.at[1]
        return jnp.where(thin_row < 4, ref[i : i + 1, :], ref[layers + i : layers + i + 1, :])

    given = {j: terms[j][7] * g_at(j) for j in terms}
    extra = {j: terms[j][0] * given[j] for j in terms}
    for width in (1, 0):
        extra = {j: thin_pass(terms, extra, j, given[j]) for j in range(-width, layers + width)}
    x_start(1, project(face_rows({l: terms[l][7] * (level[l] + extra[l] - g_at(l)) for l in range(layers)})))

    def added(l):
        d = extra[l]
        tall = jnp.concatenate(
            [jnp.where(thin_row < 4, d, 0.0), jnp.zeros((nz - 16, ny), F32), jnp.where(thin_row < 4, 0.0, d)], axis=0
        )
        return tall.T

    for l in range(layers):
        grid_d[l] = added(l)

    @pl.when(jnp.logical_not(early))
    def _():
        edges(2, True)

    for l in range(1, top):
        inner_layer(3, l)
    edge_terms(3, 0)
    edge_terms(3, 1)
    forward(3)
    x_finish(1)
    z_start(1)
    edges(3, True)
    forward(4)
    for l in range(1, top):
        inner_layer(4, l)
    edge_terms(4, 0)
    edge_terms(4, 1)
    for l in range(1, top):
        p_out[0, l] = press[5, l] + grid_d[l]
    edges(4, False)
    for l in (0, top):
        p_out[0, l] = press[5, l] + grid_d[l]
    final = mortar + z_finish(1)
    share = mort // sub_count
    offset = sub * share
    row = final[0:1, :]
    for i in range(1, rows_m):
        row = jnp.where(offset // 128 == i, final[i : i + 1, :], row)
    wide = jnp.broadcast_to(row, (8, 128))
    m_out[...] = pltpu.roll(wide, (128 - offset % 128) % 128, 1)[0:1, 0:share]

    def sent_all(copies):
        for copy in copies:
            copy.wait_send()

    on_sides(lambda side: sent_all(thin_copies(side)))
    on_sides(lambda side: near_copy(side).wait_send())
    on_sides(lambda side: g_copy(side).wait_send())

    @pl.when(has_low)
    def _():
        e1_copy(0).wait_send()
        e1_copy(1).wait_send()
        for k in range(1, 5):
            for c in range(CHUNKS):
                halo_copy(k, 0, c).wait_send()

    @pl.when(has_up)
    def _():
        e1_copy(2).wait_send()
        e1_copy(3).wait_send()
        for k in range(1, 5):
            for c in range(CHUNKS):
                halo_copy(k, 1, c).wait_send()

    @pl.when(helps_low)
    def _():
        e1_forward(0).wait_send()
        e1_forward(1).wait_send()

    @pl.when(helps_up)
    def _():
        e1_forward(2).wait_send()
        e1_forward(3).wait_send()

    @pl.when(helps)
    def _():
        for k in range(1, 5):
            if RELAYED[k] is not None:
                forward_copy(k).wait_send()

    for r in range(2):
        for i in own:
            x_copy(r, i).wait_send()
        for j in range(1, zgroups):
            z_copy(r, j).wait_send()

    @pl.when(has_prev)
    def _():
        for r in range(2):
            for i in low_block:
                x_copy(r, i).wait_send()

    @pl.when(has_next)
    def _():
        for r in range(2):
            for i in up_block:
                x_copy(r, i).wait_send()


def shards(source, trans_x, trans_y, trans_z, mortar_bot, mortar_top):
    _, layers, ny, nz = source.shape
    mort = mortar_bot.shape[3]
    sub_count = lax.axis_size("sub")
    block_count = lax.axis_size("block")
    zgroups = sub_count // GROUP
    field = pltpu.VMEM((layers, ny, nz), F32)
    basis = pltpu.VMEM((layers, ny, mort), F32)
    pair = pltpu.VMEM((2, ny, nz), F32)
    dma = pltpu.SemaphoreType.DMA
    xmsgs = 3 * GROUP - 1
    hbm = pl.BlockSpec(memory_space=pl.ANY)
    vmem = pl.BlockSpec(memory_space=pltpu.VMEM)
    return pl.pallas_call(
        functools.partial(kernel, sub_count, block_count),
        out_shape=(
            pltpu.VMEM(source.shape, F32),
            pltpu.VMEM((1, mort // sub_count), F32),
        ),
        in_specs=[hbm] * 6,
        out_specs=(vmem, vmem),
        scratch_shapes=[
            field, field, field, field, basis, basis,
            field, field, field, field, field, field, pair, field,
            pltpu.VMEM((6, layers, ny, nz), F32), pair, field,
            pltpu.VMEM((ny, nz), F32), pair, pair, pltpu.VMEM((4, 2, ny, nz), F32),
            pltpu.VMEM((2, 8, 128), F32), pltpu.VMEM((2, xmsgs, 8, 128), F32),
            pltpu.VMEM((2, 8, 128), F32), pltpu.VMEM((2, zgroups - 1, 8, 128), F32),
            pltpu.VMEM((4, (ny - 8) // (GROUP - 1), nz), F32), pltpu.VMEM((4, ny // CHUNKS, nz), F32),
            pltpu.VMEM((layers, 4, 8, ny), F32), pltpu.VMEM((2, 4, 8, ny), F32), pltpu.VMEM((3, 4, 8, ny), F32),
            pltpu.VMEM((layers, 8, ny), F32), pltpu.VMEM((3, 8, ny), F32), pltpu.VMEM((3, 8, ny), F32),
            pltpu.VMEM((2 * layers, ny), F32), pltpu.VMEM((2, 2 * layers, ny), F32),
            dma((6,)), dma((4,)), dma((4,)),
            dma((4, 2, CHUNKS)), dma((4, 2, CHUNKS)),
            dma((2, xmsgs)), dma((2, xmsgs)), dma((2, zgroups - 1)), dma((2, zgroups - 1)),
            dma((4,)), dma((4,)), dma((4,)), dma((4,)),
            dma((3,)), dma((3,)), dma((2,)), dma((2,)), dma((2,)), dma((2,)),
            pltpu.SemaphoreType.REGULAR((max(zgroups - 2, 1), 2)),
        ],
        compiler_params=pltpu.CompilerParams(collective_id=0, has_side_effects=True),
        name="mortar_darcy",
    )(source, trans_x, trans_y, trans_z, mortar_bot, mortar_top)


def solution(mesh):
    spec = P("block", "sub", None, None)
    return jax.shard_map(
        shards,
        mesh=mesh,
        in_specs=(spec,) * 6,
        out_specs=(spec, P("block", "sub")),
        check_vma=False,
    )
```
